512 devices in a mesh: tile: 2 (over y), beam: 16 (over z), bl: 8 (over x), pol: 2 (over core).
Axes of the slice: x: 8, y: 2, z: 16, core: 2. Of those that a mesh axis runs over, the one named last changes fastest.
The devices are a block of a 8x8x16 slice.
Arguments:
- sky_model: bfloat16 [4096, 16384], P(('tile', 'bl', 'pol'), 'beam'), parts along dimension 0, may hold values from -6 to 6
- beam_pattern: bfloat16 [32, 2048, 2048], P(('tile', 'beam'), ('bl', 'pol')), parts along dimension 0, may hold values from 0.099609375 to 1
- kernels: bfloat16 [32, 1024, 128, 128], P(('tile', 'beam'), ('bl', 'pol')), parts along dimension 0, may hold values from -0.5 to 0.5
- observed: float32 [32, 1024, 2, 128], P(('tile', 'beam'), ('bl', 'pol')), parts along dimension 0, may hold values from -6 to 6
- tile_owner: int32 [32, 1024, 1], P(('tile', 'beam'), ('bl', 'pol')), parts along dimension 0, may hold values from 0 to 15; in each aligned block of 64 rows (0 to 63, 64 to 127, ..., all dimensions but the last counted through in order) at most 8 rows name the same one
- tile_local: int32 [32, 1024], P(('tile', 'beam'), ('bl', 'pol')), parts along dimension 0, may hold values from 0 to 1023
- vis_count: int32 [32, 1024], P(('tile', 'beam'), ('bl', 'pol')), parts along dimension 0, may hold values from 1 to 128
Outputs:
- residual_vis: float32 [32, 1024, 2, 128], P(('tile', 'beam'), ('bl', 'pol')), parts along dimension 0
- dirty_grid: float32 [32, 16384, 2, 128], P(('tile', 'beam'), ('bl', 'pol')), parts along dimension 0
The draws below stay inside these ranges and needn't reach their ends.
There are 2 independent parts, one for each index of `tile`. The reference program is written for one: setup_inputs(seed, part) draws one part's arguments, and reference() takes and returns one part's arrays. A program takes and returns all parts, laid end to end along the dimension named above; each array names one. Nothing has to cross between parts.
Inputs may be any that keep to these rules, and one draw needn't show every extreme that they name: `tile_owner`: among the 64 visibility tiles of one device, at most 8 name the same owner, and in some blocks one owner is named exactly 8 times.
All inputs are finite; a program needn't handle non-finite values.
Results may differ from the reference program's by a relative error of at most 0.0055.
Values may be sent and summed in bfloat16 or wider, within the bound.
No kernel may reach another device: no remote copies, remote signals or barrier semaphores. Data moves between devices by JAX's collectives and lax.ppermute only.
A program may use at most 64 MiB of HBM per device.

```python
import math
import jax
import jax.numpy as jnp
import numpy as np
from jax import lax

GRID = 2048
TILE_VIS = 128
VIS_DEV = 64
BEAMS = 16
GROUP = 16
STRIDE = 1024
HALO = 512
SKY_COLS = 16384
TILES_DEV = 1024
TILES_ALL = 16384
VIS_ALL = 1024
CAP = 8


def set_ends(values, own_key, smallest, top_value):
    extent = values.shape
    index_at = [jax.random.randint(jax.random.fold_in(own_key, axis), (), 0, extent[axis]) for axis in range(len(extent))]
    values = values.at[tuple(index_at)].set(smallest)
    longest = extent.index(max(extent))
    index_at[longest] = (index_at[longest] + 1) % extent[longest]
    return values.at[tuple(index_at)].set(top_value)


def steps_of(stream_key, extent, shards, smallest, high):
    factor_of = 1.0
    for position, parts in shards:
        heights = jax.random.uniform(jax.random.fold_in(jax.random.fold_in(stream_key, 6), position), (parts,), jnp.float32, smallest / len(shards), high / len(shards))
        factor_of = factor_of * jnp.repeat(jnp.exp(heights), extent[position] // parts).reshape((-1,) + (1,) * (len(extent) - 1 - position))
    return factor_of


def shared_out(stream_key, own, number, rows, number_of, top, limit, skew):
    sequence = jax.random.permutation(stream_key, number_of)
    heavy_load, ordinary = shares(number_of, rows * top, limit, skew, True), shares(number_of, rows * top, limit, skew, False)
    places = jnp.arange(number_of)

    def named(tallies, rotation):
        used = int((tallies > 0).sum())
        fixed = max(1, used // 4)
        passed = fixed + (places - fixed + rotation * (used - fixed)) % max(1, number_of - fixed)
        return jnp.zeros((number_of,), jnp.int32).at[sequence[jnp.where(places < fixed, places, passed)]].set(jnp.asarray(tallies, jnp.int32))

    tallies = jnp.where(number % 4 == 0, named(heavy_load, number // 4), named(ordinary, number - number // 4 - 1))
    mixed = jax.random.permutation(jax.random.fold_in(own, 3), number_of)
    donor, taker = mixed[0:number_of // 2 * 2:2], mixed[1:number_of // 2 * 2:2]
    room = jnp.minimum(tallies[donor] - 1, limit - tallies[taker]) // 2
    room = jnp.where((donor == sequence[0]) | (taker == sequence[0]) | (tallies[taker] == 0), 0, jnp.maximum(room, 0))
    passed = jax.random.randint(jax.random.fold_in(own, 4), (number_of // 2,), 0, 1 << 20) % (room + 1)
    tallies = tallies.at[donor].add(-passed).at[taker].add(passed)
    items = jnp.searchsorted(jnp.cumsum(tallies), jnp.arange(rows * top), side="right").astype(jnp.int32)
    listing = items.reshape(top, rows).T
    listing = listing[jax.random.permutation(jax.random.fold_in(own, 1), rows)]
    rotation = jax.random.randint(jax.random.fold_in(own, 2), (rows, 1), 0, top)
    return jnp.take_along_axis(listing, (jnp.arange(top)[None, :] + rotation) % top, axis=1)


def shares(count, total, limit, slope, full):
    weights = [(1 << 20) // math.isqrt(rank ** slope) + 1 for rank in range(1, count + 1)]
    largest = limit if full else min(limit, max(-(-total // count), total * weights[0] // sum(weights)))
    least = 1 if total - largest >= count - 1 else 0
    given, spare = [largest] + [least] * (count - 1), total - largest - least * (count - 1)
    while spare > 0:
        free = [i for i in range(1, count) if given[i] < largest] or [i for i in range(1, count) if given[i] < limit]
        pool, left = sum([weights[i] for i in free]), spare
        for i in free:
            extra = min(limit - given[i], max(1, left * weights[i] // pool), spare)
            given[i] = given[i] + extra
            spare = spare - extra
    return np.array(given)


def scatter_about(key, dims, spread, most, split=(), held_as=jnp.bfloat16):
    array = spread * jax.random.normal(key, dims, jnp.float32)
    if split:
        array = array * steps_of(key, dims, split, -0.22, 0.18)
    return jnp.clip(array, -most, most).astype(held_as)


def setup_inputs(seed: int = 0, part: int = 0) -> dict:
    arg_keys = jax.random.split(jax.random.key(seed), 8)
    part_keys = jax.random.split(jax.random.fold_in(arg_keys[7], part), 8)
    sky_model = scatter_about(part_keys[0], (GRID, SKY_COLS), 1.0, 6.0, ((0, 16), (1, 16)))
    beam_pattern = jnp.clip(0.099609375 + 0.9003906 * jax.random.uniform(part_keys[1], (BEAMS, GRID, GRID), jnp.float32) ** steps_of(part_keys[1], (BEAMS, GRID, GRID), ((0, 16), (1, 16)), -0.2, 0.2), 0.099609375, 1.0).astype(jnp.bfloat16)
    kernels = scatter_about(part_keys[2], (BEAMS, VIS_ALL, TILE_VIS, TILE_VIS), TILE_VIS ** -0.5, 0.5, ((0, 16), (1, 16)))
    observed = scatter_about(part_keys[3], (BEAMS, VIS_ALL, 2, TILE_VIS), 1.0, 6.0, ((0, 16), (1, 16)), jnp.float32)
    tile_owner_keys = jax.random.split(jax.random.fold_in(part_keys[4], 1), BEAMS * VIS_ALL // VIS_DEV)
    tile_owner_turns = jax.random.permutation(jax.random.fold_in(part_keys[4], 3), BEAMS * VIS_ALL // VIS_DEV)
    tile_owner = jax.vmap(lambda own, number: shared_out(jax.random.fold_in(part_keys[4], 2), own, number, VIS_DEV, GROUP, 1, CAP, 2))(tile_owner_keys, tile_owner_turns).reshape((BEAMS, VIS_ALL, 1))
    tile_local = set_ends(jax.random.randint(part_keys[5], (BEAMS, VIS_ALL), 0, TILES_DEV), jax.random.fold_in(part_keys[5], 1), 0, TILES_DEV - 1).astype(jnp.int32)
    vis_count = set_ends(jax.random.randint(part_keys[6], (BEAMS, VIS_ALL), 1, TILE_VIS + 1), jax.random.fold_in(part_keys[6], 1), 1, TILE_VIS).astype(jnp.int32)
    return {"sky_model": sky_model, "beam_pattern": beam_pattern, "kernels": kernels, "observed": observed, "tile_owner": tile_owner, "tile_local": tile_local, "vis_count": vis_count}


def tables(rows, cols):
    row_index = jnp.arange(rows, dtype=jnp.int32)[:, None]
    col_index = jnp.arange(cols, dtype=jnp.int32)[None, :]
    angles = (row_index * col_index % GRID).astype(jnp.float32) * jnp.float32(2.0 * math.pi / GRID)
    factor = jnp.float32(1.0 / math.sqrt(GRID))
    return ((jnp.cos(angles) * factor).astype(jnp.bfloat16), (jnp.sin(angles) * factor).astype(jnp.bfloat16))

def product(left, right):
    return jnp.dot(left.astype(jnp.float32), right.astype(jnp.float32), precision=lax.Precision.HIGHEST)

def reference(sky_model, beam_pattern, kernels, observed, tile_owner, tile_local, vis_count):
    cos_one, sin_one = tables(GRID // 2, GRID)
    cos_two, sin_two = tables(GRID, GRID)
    padded = jnp.pad(sky_model, ((0, 0), (HALO, HALO)))

    def one_beam(packed):
        beam_no, pattern, kernel_set, seen, owners, local_ids, counts = packed
        window = lax.dynamic_slice_in_dim(padded, (beam_no * STRIDE).astype(jnp.int32), GRID, 1)
        apparent = (pattern.astype(jnp.float32) * window.astype(jnp.float32)).astype(jnp.bfloat16)
        half_real = product(cos_one, apparent.T).astype(jnp.bfloat16)
        half_imag = (-product(sin_one, apparent.T)).astype(jnp.bfloat16)
        uv_real = product(half_real, cos_two) + product(half_imag, sin_two)
        uv_imag = product(half_imag, cos_two) - product(half_real, sin_two)
        uv_grid = jnp.stack([uv_real, uv_imag]).astype(jnp.bfloat16)
        uv_tiles = uv_grid.reshape(2, GRID // 16, 8, GRID // 16, 16).transpose(1, 3, 0, 2, 4).reshape(TILES_ALL, 2, TILE_VIS)
        tile_index = (owners * TILES_DEV + local_ids).astype(jnp.int32)
        fetched = uv_tiles[tile_index]
        kernel_wide = kernel_set.astype(jnp.float32)
        predicted = jnp.einsum('rjm,rcm->rcj', kernel_wide, fetched.astype(jnp.float32), precision=lax.Precision.HIGHEST)
        live_mask = jnp.arange(TILE_VIS, dtype=jnp.int32)[None, :] < counts[:, None]
        residual = jnp.where(live_mask[:, None, :], seen - predicted, jnp.zeros_like(predicted))
        residual_low = residual.astype(jnp.bfloat16)
        contribution = jnp.einsum('rjm,rcj->rcm', kernel_wide, residual_low.astype(jnp.float32), precision=lax.Precision.HIGHEST)
        dirty = jax.ops.segment_sum(contribution, tile_index, num_segments=TILES_ALL)
        return (residual, dirty)
    beam_numbers = jnp.arange(BEAMS, dtype=jnp.int32)
    residual_vis, dirty_grid = lax.map(one_beam, (beam_numbers, beam_pattern, kernels, observed, tile_owner[:, :, 0], tile_local, vis_count))
    return (residual_vis, dirty_grid)
```

```python
import math

import jax
import jax.numpy as jnp
import numpy as np
from jax import lax
from jax.experimental import pallas as pl
from jax.experimental.pallas import tpu as pltpu
from jax.sharding import PartitionSpec as P

GRID = 2048
HALO = 512
RADIX = 16
LANES = GRID // RADIX
GROUP_AXES = ("bl", "pol")
F32 = jnp.float32
BF16 = jnp.bfloat16


def spin(re, im, k, n):
    k = k % n
    c, s = math.cos(2 * math.pi * k / n), math.sin(2 * math.pi * k / n)
    if k == 0:
        return re, im
    if 4 * k == n:
        return im, -re
    if im is None:
        return re * np.float32(c), re * np.float32(-s)
    if 8 * k == n:
        h = np.float32(math.sqrt(0.5))
        return (re + im) * h, (im - re) * h
    if 8 * k == 3 * n:
        h = np.float32(math.sqrt(0.5))
        return (im - re) * h, (re + im) * -h
    return re * np.float32(c) + im * np.float32(s), im * np.float32(c) - re * np.float32(s)


def plus(a, b):
    return b if a is None else a if b is None else a + b


def minus(a, b):
    return a if b is None else -b if a is None else a - b


def real_dft(x):
    n = len(x)
    if n == 1:
        return [(x[0], None)]
    if n == 2:
        return [(x[0] + x[1], None), (x[0] - x[1], None)]
    even, odd = real_dft(x[0::2]), real_dft(x[1::2])
    out = [None] * (n // 2 + 1)
    for k in range(n // 4 + 1):
        (er, ei), (orr, oi) = even[k], odd[k]
        if 4 * k == n:
            tr, ti = None, (None if orr is None else -orr)
        else:
            tr, ti = spin(orr, oi, k, n)
        out[k] = (plus(er, tr), plus(ei, ti))
        if n // 2 - k != k:
            low = minus(ei, ti)
            out[n // 2 - k] = (minus(er, tr), None if low is None else minus(None, low))
    return out


def complex_dft(x):
    n = len(x)
    if n == 1:
        return x
    even, odd = complex_dft(x[0::2]), complex_dft(x[1::2])
    low, high = [], []
    for k in range(n // 2):
        (er, ei), (tr, ti) = even[k], spin(odd[k][0], odd[k][1], k, n)
        low.append((er + tr, ei + ti))
        high.append((er - tr, ei - ti))
    return low + high


def first_table(group):
    half = RADIX // 2
    per = GRID // 2 // RADIX // group
    p, d, s, q = np.meshgrid(
        np.arange(half), np.arange(group), np.arange(2), np.arange(per), indexing="ij"
    )
    u1 = np.where(s == 0, p, np.where(p == 0, half, RADIX - p))
    u = RADIX * (per * d + q) + u1
    x0 = np.arange(LANES)
    angle = 2 * np.pi * ((u[..., None] * x0) % GRID) / GRID
    c, n = np.cos(angle) / math.sqrt(GRID), np.sin(angle) / math.sqrt(GRID)
    first = (p == 0)[..., None]
    side = (s == 0)[..., None]
    sign = np.where(side, 1.0, -1.0)
    rr = np.where(first, np.where(side, c, 0.0), c)
    ri = np.where(first, np.where(side, 0.0, c), sign * n)
    ir = np.where(first, np.where(side, -n, 0.0), -n)
    ii = np.where(first, np.where(side, 0.0, -n), sign * c)
    real = np.concatenate([rr, ri], axis=-1)
    imag = np.concatenate([ir, ii], axis=-1)
    both = np.stack([real, imag], axis=2)
    return both.reshape(half, group * 2 * 2 * per, 2 * LANES).astype(np.float32).astype(BF16)


def second_table():
    v1, y0, v0 = np.meshgrid(np.arange(RADIX), np.arange(LANES), np.arange(LANES), indexing="ij")
    angle = 2 * np.pi * ((y0 * (RADIX * v0 + v1)) % GRID) / GRID
    c, n = np.cos(angle) / math.sqrt(GRID), np.sin(angle) / math.sqrt(GRID)
    top = np.concatenate([c, -n], axis=2)
    low = np.concatenate([n, c], axis=2)
    return np.concatenate([top, low], axis=1).astype(np.float32).astype(BF16)


def placing(rows):
    row = np.arange(rows)
    p, s = row // 8, (row // 4) % 2
    i = np.where(s == 0, p, (8 - p) % 8)
    out = np.zeros((8 * RADIX, RADIX, rows), np.float32)
    for v1 in range(RADIX):
        out[RADIX * i + v1, v1, row] = 1.0
    return out.reshape(8 * RADIX, RADIX * rows).astype(BF16)


def dot(a, b, dims=((1,), (0,))):
    return lax.dot_general(a, b, (dims, ((), ())), preferred_element_type=F32)


def iota(shape, dim):
    return lax.broadcasted_iota(jnp.int32, shape, dim)


def plan_body(
    owner_ref, local_ref, count_ref, sky_any, pattern_any, table_any,
    ids_ref, pick_ref, put_ref, live_ref, sky_ref, pattern_ref, table_ref, sems,
):
    copies = [
        pltpu.make_async_copy(source, target, sems.at[i])
        for i, (source, target) in enumerate(
            [(sky_any, sky_ref), (pattern_any, pattern_ref), (table_any, table_ref)]
        )
    ]
    for copy in copies:
        copy.start()
    n = owner_ref.shape[0]
    group, cap = ids_ref.shape
    owner_col = owner_ref[...].astype(F32)
    local_row = local_ref[...].astype(F32)
    count_row = count_ref[...].astype(F32)
    eye = iota((n, n), 0) == iota((n, n), 1)
    owner_row = jnp.sum(jnp.where(eye, owner_col, 0.0), axis=0, keepdims=True)
    same = owner_col == owner_row
    before = jnp.where(same & (iota((n, n), 0) < iota((n, n), 1)), 1.0, 0.0)
    slot_row = jnp.sum(before, axis=0, keepdims=True)
    after = jnp.where(same & (iota((n, n), 1) < iota((n, n), 0)), 1.0, 0.0)
    slot_col = jnp.sum(after, axis=1, keepdims=True)
    mine = iota((group, n), 0).astype(F32) == owner_row
    ids = jnp.zeros((group, cap), F32)
    for k in range(cap):
        hit = jnp.where(mine & (slot_row == float(k)), local_row + 1.0, 0.0)
        ids = jnp.where(iota((group, cap), 1) == k, jnp.sum(hit, axis=1, keepdims=True), ids)
    ids_ref[...] = ids.astype(jnp.int32) - 1
    target_row = owner_row * float(2 * cap) + slot_row
    target_col = owner_col * float(2 * cap) + slot_col
    rows, wide = pick_ref.shape
    mid = jnp.where(iota((rows, n), 0) // 2 == iota((rows, n), 1), 1.0, 0.0)
    col = jnp.sum(mid * target_row, axis=1, keepdims=True)
    col = col + (iota((rows, 1), 0) % 2 * cap).astype(F32)
    pick_ref[...] = jnp.where(iota((rows, wide), 1).astype(F32) == col, 1.0, 0.0).astype(BF16)
    dim = jnp.where(iota((n, rows), 1) // 2 == iota((n, rows), 0), 1.0, 0.0)
    row = jnp.sum(dim * target_col, axis=0, keepdims=True)
    row = row + (iota((1, rows), 1) % 2 * cap).astype(F32)
    put_ref[...] = jnp.where(iota((wide, rows), 0).astype(F32) == row, 1.0, 0.0).astype(BF16)
    count = jnp.sum(mid * count_row, axis=1, keepdims=True)
    live_ref[...] = jnp.where(iota(live_ref.shape, 1).astype(F32) < count, 1.0, 0.0)
    for copy in copies:
        copy.wait()


def first_body(low_ref, sky_ref, high_ref, pattern_ref, table_ref, out_any, mid_ref, out_ref, sems):
    rows = sky_ref.shape[0]
    block = 16
    for start in range(0, rows, block):
        at = slice(start, start + block)
        parts = []
        for x1 in range(RADIX):
            lo = x1 * LANES
            if lo < HALO:
                sky = low_ref[at, lo : lo + LANES]
            elif lo < GRID - HALO:
                sky = sky_ref[at, lo - HALO : lo - HALO + LANES]
            else:
                sky = high_ref[at, lo - GRID + HALO : lo - GRID + HALO + LANES]
            seen = pattern_ref[at, lo : lo + LANES].astype(F32) * sky.astype(F32)
            parts.append(seen.astype(BF16).astype(F32))
        out = real_dft(parts)
        mid_ref[0, at, :LANES] = out[0][0].astype(BF16)
        mid_ref[0, at, LANES:] = out[RADIX // 2][0].astype(BF16)
        for p in range(1, RADIX // 2):
            mid_ref[p, at, :LANES] = out[p][0].astype(BF16)
            mid_ref[p, at, LANES:] = out[p][1].astype(BF16)
    group = out_ref.shape[1]
    copies = []
    for p in range(RADIX // 2):
        half = dot(table_ref[p], mid_ref[p], ((1,), (1,)))
        per = half.shape[0] // group
        out_ref[p] = half.reshape(group, per, rows).astype(BF16)
        copies.append(
            pltpu.make_async_copy(
                out_ref.at[p], out_any.at[:, p * per : (p + 1) * per, :], sems.at[p]
            )
        )
        copies[-1].start()
    for copy in copies:
        copy.wait()


def second_body(half_ref, ids_ref, table_any, place_any, out_ref, table_ref, place_ref, mid_ref, sel_ref, sems):
    copies = [
        pltpu.make_async_copy(table_any.at[v1], table_ref.at[v1], sems.at[v1])
        for v1 in range(RADIX)
    ]
    copies.append(pltpu.make_async_copy(place_any, place_ref, sems.at[RADIX]))
    for copy in copies:
        copy.start()
    group = half_ref.shape[0]
    rows = mid_ref.shape[1]
    for pair in range(rows // 16):
        done = []
        for p in (2 * pair, 2 * pair + 1):
            parts = []
            for y1 in range(group):
                both = half_ref[y1, 16 * p : 16 * p + 16, :].astype(F32)
                parts.append((both[:8], both[8:]))
            done.append(complex_dft(parts))
        at = slice(16 * pair, 16 * pair + 16)
        for v1 in range(RADIX):
            for c in range(2):
                both = jnp.concatenate([done[0][v1][c], done[1][v1][c]], axis=0)
                mid_ref[v1, at, c * LANES : (c + 1) * LANES] = both.astype(BF16)
    ids = ids_ref[...]
    wanted = ids.shape[1]
    hot = jnp.where(iota((LANES, wanted), 0) == ids % LANES, 1.0, 0.0).astype(BF16)
    row = iota((rows, wanted), 0)
    mask = jnp.where(2 * (row % 4) + row // 4 % 2 == ids // LANES, 1.0, 0.0)
    for v1 in range(RADIX):
        copies[v1].wait()
        grid = dot(mid_ref[v1], table_ref[v1]).astype(BF16)
        for c in range(2):
            got = dot(grid[:, c * LANES : (c + 1) * LANES], hot)
            sel_ref[c, v1 * rows : (v1 + 1) * rows, :] = (got * mask).astype(BF16)
    copies[RADIX].wait()
    tiles = []
    for c in range(2):
        got = dot(place_ref[...], sel_ref[c])
        tiles.append(got.T.reshape(group, wanted // group, got.shape[0]))
    out_ref[...] = jnp.concatenate(tiles, axis=1).astype(BF16)


def visit_body(
    tiles_ref, pick_ref, put_ref, live_ref, seen_ref, kernel_any, res_ref, out_ref, kernel_ref, sems
):
    cells = kernel_ref.shape[1]
    rows = seen_ref.shape[0]
    size = 4 * cells
    copies = [
        pltpu.make_async_copy(
            kernel_any.at[pl.ds(g * size, size)], kernel_ref.at[pl.ds(g * size, size)], sems.at[g]
        )
        for g in range(rows // 8)
    ]
    for copy in copies:
        copy.start()
    fetched = dot(pick_ref[...], tiles_ref[...])
    of = iota((8, cells), 0) // 2
    terms = []
    for g in range(rows // 8):
        at = slice(8 * g, 8 * g + 8)
        own = fetched[at]
        guess = jnp.zeros((8, cells), F32)
        copies[g].wait()
        for h in range(2):
            left = jnp.concatenate(
                [jnp.where(of == 2 * h + q, own, 0.0) for q in range(2)], axis=1
            ).astype(BF16)
            first = (4 * g + 2 * h) * cells
            right = jnp.concatenate(
                [kernel_ref[first : first + cells], kernel_ref[first + cells : first + 2 * cells]],
                axis=1,
            )
            guess = guess + dot(left, right, ((1,), (1,)))
        res = jnp.where(live_ref[at] > 0.0, seen_ref[at] - guess, 0.0)
        res_ref[at] = res
        term = jnp.zeros((8, cells), F32)
        for h in range(2):
            left = jnp.concatenate(
                [jnp.where(of == 2 * h + q, res, 0.0) for q in range(2)], axis=1
            ).astype(BF16)
            first = (4 * g + 2 * h) * cells
            term = term + dot(left, kernel_ref[first : first + 2 * cells])
        terms.append(term)
    term = jnp.concatenate(terms, axis=0).astype(BF16)
    out_ref[...] = dot(put_ref[...], term).astype(BF16)


def dirty_body(term_ref, target_ref, out_any, out_ref, sems):
    rows = out_ref.shape[0]
    step = rows // sems.shape[0]
    target = target_ref[...]
    term = term_ref[...]
    copies = []
    for i in range(sems.shape[0]):
        at = pl.ds(i * step, step)
        hot = jnp.where(iota((step, target.shape[1]), 0) + i * step == target, 1.0, 0.0)
        out_ref[at, :] = dot(hot.astype(BF16), term)
        copies.append(pltpu.make_async_copy(out_ref.at[at], out_any.at[at], sems.at[i]))
        copies[-1].start()
    for copy in copies:
        copy.wait()


FAST = pltpu.VMEM
ANY = pl.ANY


def call(body, name, outs, args, scratch=()):
    shapes = [
        pltpu.VMEM(s, d) if space is FAST else jax.ShapeDtypeStruct(s, d) for s, d, space in outs
    ]
    spec = lambda space: pl.BlockSpec(memory_space=pltpu.VMEM if space is None else space)
    return pl.pallas_call(
        body,
        out_shape=shapes,
        in_specs=[spec(space) for _, space in args],
        out_specs=[spec(space) for _, _, space in outs],
        scratch_shapes=list(scratch),
        name=name,
    )(*[pltpu.with_memory_space_constraint(a, FAST) if space is FAST else a for a, space in args])


def exchange(block):
    return lax.all_to_all(block, GROUP_AXES, split_axis=0, concat_axis=0, tiled=True)


def on_device(sky_model, beam_pattern, kernels, observed, tile_owner, tile_local, vis_count):
    group = lax.axis_size(GROUP_AXES)
    rows, strip = sky_model.shape
    vis, cells = kernels.shape[1], kernels.shape[3]
    cap = max(2, 2 * vis // group)
    u_rows = GRID // 2 // group
    tiles_dev = u_rows // 8 * (GRID // 16)
    sem = pltpu.SemaphoreType.DMA

    count = lax.axis_size("beam")
    forward = [(i, i + 1) for i in range(count - 1)]
    backward = [(target, source) for source, target in forward]
    low = lax.ppermute(sky_model[:, strip - HALO :], "beam", forward)
    high = lax.ppermute(sky_model[:, :HALO], "beam", backward)

    table = first_table(group)
    ids, pick, put, live, sky_fast, pattern_fast, table_fast = call(
        plan_body,
        "plan",
        [
            ((group, cap), jnp.int32, None),
            ((2 * vis, 2 * group * cap), BF16, FAST),
            ((2 * group * cap, 2 * vis), BF16, FAST),
            ((2 * vis, cells), F32, FAST),
            ((rows, strip), BF16, FAST),
            ((rows, GRID), BF16, FAST),
            (table.shape, BF16, FAST),
        ],
        [
            (tile_owner[0], None),
            (tile_local, None),
            (vis_count, None),
            (sky_model, ANY),
            (beam_pattern[0], ANY),
            (table, ANY),
        ],
        [sem((3,))],
    )
    asked = exchange(ids)
    asked_row = asked.reshape(1, group * cap)
    target = jnp.concatenate([2 * asked, 2 * asked + 1], axis=1).reshape(1, 2 * group * cap)

    (half,) = call(
        first_body,
        "first",
        [((group, 2 * u_rows, rows), BF16, ANY)],
        [(low, FAST), (sky_fast, FAST), (high, FAST), (pattern_fast, FAST), (table_fast, FAST)],
        [
            pltpu.VMEM((RADIX // 2, rows, 2 * LANES), BF16),
            pltpu.VMEM((RADIX // 2, group, 2 * u_rows // 8, rows), BF16),
            sem((RADIX // 2,)),
        ],
    )
    columns = exchange(half)
    table = second_table()
    place = placing(u_rows)
    (tiles,) = call(
        second_body,
        "second",
        [((group, 2 * cap, cells), BF16, None)],
        [(columns, FAST), (asked_row, FAST), (table, ANY), (place, ANY)],
        [
            pltpu.VMEM(table.shape, BF16),
            pltpu.VMEM(place.shape, BF16),
            pltpu.VMEM((RADIX, u_rows, 2 * LANES), BF16),
            pltpu.VMEM((2, RADIX * u_rows, group * cap), BF16),
            sem((RADIX + 1,)),
        ],
    )
    returned = exchange(tiles)
    residual, terms = call(
        visit_body,
        "visit",
        [((2 * vis, cells), F32, None), ((2 * group * cap, cells), BF16, None)],
        [
            (returned.reshape(2 * group * cap, cells), FAST),
            (pick, FAST),
            (put, FAST),
            (live, FAST),
            (observed.reshape(2 * vis, cells), FAST),
            (kernels.reshape(vis * cells, cells), ANY),
        ],
        [pltpu.VMEM((vis * cells, cells), BF16), sem((vis // 4,))],
    )
    arrived = exchange(terms.reshape(group, 2 * cap, cells))
    (dirty,) = call(
        dirty_body,
        "dirty",
        [((2 * tiles_dev, cells), F32, ANY)],
        [(arrived.reshape(2 * group * cap, cells), FAST), (target, FAST)],
        [pltpu.VMEM((2 * tiles_dev, cells), F32), sem((8,))],
    )
    return residual.reshape(1, vis, 2, cells), dirty.reshape(1, tiles_dev, 2, cells)


def solution(mesh):
    placed = (
        P(("tile", "bl", "pol"), "beam"),
        P(("tile", "beam"), ("bl", "pol"), None),
        P(("tile", "beam"), ("bl", "pol"), None, None),
        P(("tile", "beam"), ("bl", "pol"), None, None),
        P(("tile", "beam"), ("bl", "pol"), None),
        P(("tile", "beam"), ("bl", "pol")),
        P(("tile", "beam"), ("bl", "pol")),
    )
    return jax.shard_map(
        on_device,
        mesh=mesh,
        in_specs=placed,
        out_specs=(
            P(("tile", "beam"), ("bl", "pol"), None, None),
            P(("tile", "beam"), ("bl", "pol"), None, None),
        ),
        check_vma=False,
    )
```

```python
import math

import jax
import jax.numpy as jnp
import numpy as np
from jax import lax
from jax.experimental import pallas as pl
from jax.experimental.pallas import tpu as pltpu
from jax.sharding import PartitionSpec as P

GRID = 2048
HALO = 512
RADIX = 16
LANES = GRID // RADIX
GROUP_AXES = ("bl", "pol")
F32 = jnp.float32
BF16 = jnp.bfloat16


def spin(re, im, k, n):
    k = k % n
    c, s = math.cos(2 * math.pi * k / n), math.sin(2 * math.pi * k / n)
    if k == 0:
        return re, im
    if 4 * k == n:
        return im, -re
    if im is None:
        return re * np.float32(c), re * np.float32(-s)
    if 8 * k == n:
        h = np.float32(math.sqrt(0.5))
        return (re + im) * h, (im - re) * h
    if 8 * k == 3 * n:
        h = np.float32(math.sqrt(0.5))
        return (im - re) * h, (re + im) * -h
    return re * np.float32(c) + im * np.float32(s), im * np.float32(c) - re * np.float32(s)


def plus(a, b):
    return b if a is None else a if b is None else a + b


def minus(a, b):
    return a if b is None else -b if a is None else a - b


def real_dft(x):
    n = len(x)
    if n == 1:
        return [(x[0], None)]
    if n == 2:
        return [(x[0] + x[1], None), (x[0] - x[1], None)]
    even, odd = real_dft(x[0::2]), real_dft(x[1::2])
    out = [None] * (n // 2 + 1)
    for k in range(n // 4 + 1):
        (er, ei), (orr, oi) = even[k], odd[k]
        if 4 * k == n:
            tr, ti = None, (None if orr is None else -orr)
        else:
            tr, ti = spin(orr, oi, k, n)
        out[k] = (plus(er, tr), plus(ei, ti))
        if n // 2 - k != k:
            low = minus(ei, ti)
            out[n // 2 - k] = (minus(er, tr), None if low is None else minus(None, low))
    return out


def first_table():
    half = RADIX // 2
    p, s, u0 = np.meshgrid(
        np.arange(half), np.arange(2), np.arange(GRID // 2 // RADIX), indexing="ij"
    )
    u1 = np.where(s == 0, p, np.where(p == 0, half, RADIX - p))
    u = RADIX * u0 + u1
    x0 = np.arange(LANES)
    angle = 2 * np.pi * ((u[..., None] * x0) % GRID) / GRID
    c, n = np.cos(angle) / math.sqrt(GRID), np.sin(angle) / math.sqrt(GRID)
    first = (p == 0)[..., None]
    side = (s == 0)[..., None]
    sign = np.where(side, 1.0, -1.0)
    rr = np.where(first, np.where(side, c, 0.0), c)
    ri = np.where(first, np.where(side, 0.0, c), sign * n)
    ir = np.where(first, np.where(side, -n, 0.0), -n)
    ii = np.where(first, np.where(side, 0.0, -n), sign * c)
    real = np.concatenate([rr, ri], axis=-1)
    imag = np.concatenate([ir, ii], axis=-1)
    both = np.stack([real, imag], axis=1)
    return both.reshape(half, 2 * GRID // RADIX, 2 * LANES).astype(np.float32).astype(BF16)


def turn_table():
    angle = 2 * np.pi * (np.outer(np.arange(LANES), np.arange(LANES)) % LANES) / LANES
    return np.stack([np.cos(angle), np.sin(angle)]).astype(np.float32)


def mix_table(group):
    y = np.arange(group * LANES).reshape(group, LANES, 1)
    angle = 2 * np.pi * ((y * np.arange(RADIX)) % GRID) / GRID
    c, n = np.cos(angle) / math.sqrt(GRID), np.sin(angle) / math.sqrt(GRID)
    top = np.concatenate([c, -n], axis=2)
    low = np.concatenate([n, c], axis=2)
    both = np.concatenate([top, low], axis=1)
    return np.tile(both, (1, 1, LANES // (2 * RADIX))).astype(np.float32).astype(BF16)


def dot(a, b, dims=((1,), (0,))):
    return lax.dot_general(a, b, (dims, ((), ())), preferred_element_type=F32)


def iota(shape, dim):
    return lax.broadcasted_iota(jnp.int32, shape, dim)


def plan_body(
    owner_ref, count_ref, sky_any, pattern_any, table_any,
    put_ref, live_ref, sky_ref, pattern_ref, table_ref, sems,
):
    copies = [
        pltpu.make_async_copy(source, target, sems.at[i])
        for i, (source, target) in enumerate(
            [(sky_any, sky_ref), (pattern_any, pattern_ref), (table_any, table_ref)]
        )
    ]
    for copy in copies:
        copy.start()
    n = owner_ref.shape[1]
    wide, rows = put_ref.shape
    cap = wide // (2 * GRID // LANES)
    owner_row = owner_ref[...].astype(F32)
    count_row = count_ref[...].astype(F32)
    eye = iota((n, n), 0) == iota((n, n), 1)
    owner_col = jnp.sum(jnp.where(eye, owner_row, 0.0), axis=1, keepdims=True)
    after = jnp.where((owner_col == owner_row) & (iota((n, n), 1) < iota((n, n), 0)), 1.0, 0.0)
    slot_col = jnp.sum(after, axis=1, keepdims=True)
    target_col = owner_col * float(2 * cap) + slot_col
    spread = jnp.where(iota((n, rows), 1) // 2 == iota((n, rows), 0), 1.0, 0.0)
    row = jnp.sum(spread * target_col, axis=0, keepdims=True)
    row = row + (iota((1, rows), 1) % 2 * cap).astype(F32)
    put_ref[...] = jnp.where(iota((wide, rows), 0).astype(F32) == row, 1.0, 0.0).astype(BF16)
    double = jnp.where(iota((rows, n), 0) // 2 == iota((rows, n), 1), 1.0, 0.0)
    count = jnp.sum(double * count_row, axis=1, keepdims=True)
    live_ref[...] = jnp.where(iota(live_ref.shape, 1).astype(F32) < count, 1.0, 0.0)
    for copy in copies:
        copy.wait()


def sky_body(
    me_ref, asked_ref, low_ref, sky_ref, high_ref, pattern_ref, table_ref, turn_any, mix_any,
    out_any, mid_ref, half_ref, left_ref, turn_ref, mix_ref, wide_ref, out_ref, asked_smem, sems,
):
    ids = pltpu.make_async_copy(asked_ref, asked_smem, sems.at[0])
    turn = pltpu.make_async_copy(turn_any, turn_ref, sems.at[1])
    mix = pltpu.make_async_copy(mix_any.at[me_ref[0]], mix_ref, sems.at[2])
    for copy in (ids, turn, mix):
        copy.start()
    rows = sky_ref.shape[0]
    block = 16
    for start in range(0, rows, block):
        at = slice(start, start + block)
        parts = []
        for x1 in range(RADIX):
            lo = x1 * LANES
            if lo < HALO:
                sky = low_ref[at, lo : lo + LANES]
            elif lo < GRID - HALO:
                sky = sky_ref[at, lo - HALO : lo - HALO + LANES]
            else:
                sky = high_ref[at, lo - GRID + HALO : lo - GRID + HALO + LANES]
            seen = pattern_ref[at, lo : lo + LANES].astype(F32) * sky.astype(F32)
            parts.append(seen.astype(BF16).astype(F32))
        out = real_dft(parts)
        mid_ref[0, at, :LANES] = out[0][0].astype(BF16)
        mid_ref[0, at, LANES:] = out[RADIX // 2][0].astype(BF16)
        for p in range(1, RADIX // 2):
            mid_ref[p, at, :LANES] = out[p][0].astype(BF16)
            mid_ref[p, at, LANES:] = out[p][1].astype(BF16)
    per = GRID // 2 // RADIX
    for p in range(RADIX // 2):
        half = dot(table_ref[p], mid_ref[p], ((1,), (1,))).astype(BF16).astype(F32)
        for c in range(2):
            for s in range(2):
                i = p if s == 0 else (8 - p) % 8
                first = (2 * c + s) * per
                half_ref[pl.ds(16 * s + 8 * c + i, per, stride=32), :] = half[first : first + per]
    mix.wait()
    quarter = LANES // 4
    for q in range(4):
        held = mix_ref[...].astype(F32)
        lane = iota(held.shape, 1) // quarter == q
        wide_ref[2 * LANES * q : 2 * LANES * (q + 1), :] = jnp.where(lane, held, 0.0).astype(BF16)
    ids.wait()
    turn.wait()
    group, vis = asked_ref.shape
    steps = vis // 8

    def step(n, carry):
        dest, first = n // steps, n % steps * 8
        both = []
        for r in range(8):
            tile = asked_smem[dest, first + r]
            at = pl.multiple_of(tile // LANES * 16, 16)
            v0 = tile % LANES
            re, im = half_ref[pl.ds(at, 8), :], half_ref[pl.ds(at + 8, 8), :]
            c, s = turn_ref[0, pl.ds(v0, 1), :], turn_ref[1, pl.ds(v0, 1), :]
            both.append((re * c + im * s, im * c - re * s))
        at = pl.ds(pl.multiple_of(n * 16, 16), 16)
        for q in range(4):
            for part in range(2):
                lo = (2 * q + part) * LANES
                pair = jnp.concatenate([both[q][part], both[q + 4][part]], axis=0)
                left_ref[at, lo : lo + LANES] = pair.astype(BF16)
        return carry

    lax.fori_loop(0, group * steps, step, 0, unroll=4)
    copies = []
    chunk = 256
    for i in range(group * vis * 2 // chunk):
        at = pl.ds(i * chunk, chunk)
        out_ref[at, :] = dot(left_ref[at, :], wide_ref[...]).astype(BF16)
        copies.append(pltpu.make_async_copy(out_ref.at[at], out_any.at[at], sems.at[3 + i]))
        copies[-1].start()
    for copy in copies:
        copy.wait()


def target_body(me_ref, asked_ref, kernel_any, target_ref, kernel_ref, sem):
    copy = pltpu.make_async_copy(kernel_any, kernel_ref, sem)
    copy.start()
    group, n = asked_ref.shape
    wide = target_ref.shape[1]
    cap = wide // (2 * group)
    asked = asked_ref[...]
    each = LANES * 8
    mine = asked // each == me_ref[0]
    local = (asked % each).astype(F32)
    before = jnp.where(iota((n, n), 0) < iota((n, n), 1), 1.0, 0.0).astype(BF16)
    slot = dot(jnp.where(mine, 1.0, 0.0).astype(BF16), before)
    lane = iota((group, wide), 1)
    found = jnp.zeros((group, wide), F32)
    for k in range(cap):
        hit = jnp.where(mine & (slot == float(k)), local + 1.0, 0.0)
        found = jnp.where(lane % cap == k, jnp.sum(hit, axis=1, keepdims=True), found)
    found = 2.0 * (found - 1.0) + (lane // cap % 2).astype(F32)
    own = lane // (2 * cap) == iota((group, wide), 0)
    target_ref[...] = jnp.sum(jnp.where(own, found, 0.0), axis=0, keepdims=True).astype(jnp.int32)
    copy.wait()


def swap_blocks(x):
    sub, block = iota(x.shape, 0), iota(x.shape, 1) // RADIX
    for bit in (1, 2, 4):
        up = pltpu.roll(pltpu.roll(x, 8 - bit, 0), RADIX * bit, 1)
        down = pltpu.roll(pltpu.roll(x, bit, 0), LANES - RADIX * bit, 1)
        s, b = sub & bit, block & bit
        x = jnp.where(s == b, x, jnp.where(s == 0, up, down))
    return x


def visit_body(tiles_ref, put_ref, live_ref, seen_ref, kernel_ref, res_ref, out_ref):
    cells = kernel_ref.shape[1]
    rows = seen_ref.shape[0]
    of = iota((8, cells), 0) // 2

    def left(own, h):
        return jnp.concatenate(
            [jnp.where(of == 2 * h + q, own, 0.0) for q in range(2)], axis=1
        ).astype(BF16)

    blocks = range(rows // 8)
    guesses = []
    for g in blocks:
        at = slice(8 * g, 8 * g + 8)
        total = tiles_ref[0, at].astype(F32)
        for source in range(1, tiles_ref.shape[0]):
            total = total + tiles_ref[source, at].astype(F32)
        own = swap_blocks(total.astype(BF16).astype(F32))
        guess = None
        for h in range(2):
            first = (4 * g + 2 * h) * cells
            right = jnp.concatenate(
                [kernel_ref[first : first + cells], kernel_ref[first + cells : first + 2 * cells]],
                axis=1,
            )
            guess = plus(guess, dot(left(own, h), right, ((1,), (1,))))
        guesses.append(guess)
    res = jnp.where(live_ref[...] > 0.0, seen_ref[...] - jnp.concatenate(guesses, axis=0), 0.0)
    res_ref[...] = res
    terms = []
    for g in blocks:
        own = res[8 * g : 8 * g + 8]
        term = None
        for h in range(2):
            first = (4 * g + 2 * h) * cells
            term = plus(term, dot(left(own, h), kernel_ref[first : first + 2 * cells]))
        terms.append(term)
    term = jnp.concatenate(terms, axis=0).astype(BF16)
    out_ref[...] = dot(put_ref[...], term).astype(BF16)


def dirty_body(term_ref, target_ref, out_any, out_ref, sems):
    rows = out_ref.shape[0]
    step = rows // sems.shape[0]
    target = target_ref[...]
    term = term_ref[...]
    copies = []
    for i in range(sems.shape[0]):
        at = pl.ds(i * step, step)
        hot = jnp.where(iota((step, target.shape[1]), 0) + i * step == target, 1.0, 0.0)
        out_ref[at, :] = dot(hot.astype(BF16), term)
        copies.append(pltpu.make_async_copy(out_ref.at[at], out_any.at[at], sems.at[i]))
        copies[-1].start()
    for copy in copies:
        copy.wait()


FAST = pltpu.VMEM
ANY = pl.ANY


def call(body, name, outs, args, scratch=()):
    shapes = [
        pltpu.VMEM(s, d) if space is FAST else jax.ShapeDtypeStruct(s, d) for s, d, space in outs
    ]
    spec = lambda space: pl.BlockSpec(memory_space=pltpu.VMEM if space is None else space)
    return pl.pallas_call(
        body,
        out_shape=shapes,
        in_specs=[spec(space) for _, space in args],
        out_specs=[spec(space) for _, _, space in outs],
        scratch_shapes=list(scratch),
        name=name,
    )(*[pltpu.with_memory_space_constraint(a, FAST) if space is FAST else a for a, space in args])


def exchange(block):
    return lax.all_to_all(block, GROUP_AXES, split_axis=0, concat_axis=0, tiled=True)


def on_device(sky_model, beam_pattern, kernels, observed, tile_owner, tile_local, vis_count):
    group = lax.axis_size(GROUP_AXES)
    rows, strip = sky_model.shape
    vis, cells = kernels.shape[1], kernels.shape[3]
    cap = max(2, 2 * vis // group)
    u_rows = GRID // 2 // group
    tiles_dev = u_rows // 8 * (GRID // 16)
    sem = pltpu.SemaphoreType.DMA
    me = lax.axis_index(GROUP_AXES).astype(jnp.int32).reshape(1)

    numbers = tile_owner[:, :, 0] * tiles_dev + tile_local
    asked = exchange(jnp.broadcast_to(numbers, (group, vis)))

    count = lax.axis_size("beam")
    forward = [(i, i + 1) for i in range(count - 1)]
    backward = [(target, source) for source, target in forward]
    low = lax.ppermute(sky_model[:, strip - HALO :], "beam", forward)
    high = lax.ppermute(sky_model[:, :HALO], "beam", backward)

    table = first_table()
    put, live, sky_fast, pattern_fast, table_fast = call(
        plan_body,
        "plan",
        [
            ((2 * group * cap, 2 * vis), BF16, FAST),
            ((2 * vis, cells), F32, FAST),
            ((rows, strip), BF16, FAST),
            ((rows, GRID), BF16, FAST),
            (table.shape, BF16, FAST),
        ],
        [
            (tile_owner[:, :, 0], None),
            (vis_count, None),
            (sky_model, ANY),
            (beam_pattern[0], ANY),
            (table, ANY),
        ],
        [sem((3,))],
    )
    turn, mix = turn_table(), mix_table(group)
    (partial,) = call(
        sky_body,
        "sky",
        [((group * 2 * vis, cells), BF16, ANY)],
        [
            (me, pltpu.SMEM),
            (asked, FAST),
            (low, FAST),
            (sky_fast, FAST),
            (high, FAST),
            (pattern_fast, FAST),
            (table_fast, FAST),
            (turn, ANY),
            (mix, ANY),
        ],
        [
            pltpu.VMEM((RADIX // 2, rows, 2 * LANES), BF16),
            pltpu.VMEM((GRID, LANES), F32),
            pltpu.VMEM((group * 2 * vis, 8 * LANES), BF16),
            pltpu.VMEM(turn.shape, F32),
            pltpu.VMEM(mix.shape[1:], BF16),
            pltpu.VMEM((8 * LANES, LANES), BF16),
            pltpu.VMEM((group * 2 * vis, cells), BF16),
            pltpu.SMEM((group, vis), jnp.int32),
            sem((3 + group * 2 * vis // 256,)),
        ],
    )
    tiles = exchange(partial.reshape(group, 2 * vis, cells))
    target, kernels_fast = call(
        target_body,
        "target",
        [((1, 2 * group * cap), jnp.int32, FAST), ((vis * cells, cells), BF16, FAST)],
        [(me, pltpu.SMEM), (asked, FAST), (kernels.reshape(vis * cells, cells), ANY)],
        [sem],
    )
    residual, terms = call(
        visit_body,
        "visit",
        [((2 * vis, cells), F32, None), ((2 * group * cap, cells), BF16, None)],
        [
            (tiles, FAST),
            (put, FAST),
            (live, FAST),
            (observed.reshape(2 * vis, cells), FAST),
            (kernels_fast, FAST),
        ],
    )
    arrived = exchange(terms.reshape(group, 2 * cap, cells))
    (dirty,) = call(
        dirty_body,
        "dirty",
        [((2 * tiles_dev, cells), F32, ANY)],
        [(arrived.reshape(2 * group * cap, cells), FAST), (target, FAST)],
        [pltpu.VMEM((2 * tiles_dev, cells), F32), sem((8,))],
    )
    return residual.reshape(1, vis, 2, cells), dirty.reshape(1, tiles_dev, 2, cells)


def solution(mesh):
    placed = (
        P(("tile", "bl", "pol"), "beam"),
        P(("tile", "beam"), ("bl", "pol"), None),
        P(("tile", "beam"), ("bl", "pol"), None, None),
        P(("tile", "beam"), ("bl", "pol"), None, None),
        P(("tile", "beam"), ("bl", "pol"), None),
        P(("tile", "beam"), ("bl", "pol")),
        P(("tile", "beam"), ("bl", "pol")),
    )
    return jax.shard_map(
        on_device,
        mesh=mesh,
        in_specs=placed,
        out_specs=(
            P(("tile", "beam"), ("bl", "pol"), None, None),
            P(("tile", "beam"), ("bl", "pol"), None, None),
        ),
        check_vma=False,
    )
```

```python
import math

import jax
import jax.numpy as jnp
import numpy as np
from jax import lax
from jax.experimental import pallas as pl
from jax.experimental.pallas import tpu as pltpu
from jax.sharding import PartitionSpec as P

GRID = 2048
HALO = 512
RADIX = 16
LANES = GRID // RADIX
GROUP_AXES = ("bl", "pol")
F32 = jnp.float32
BF16 = jnp.bfloat16


def spin(re, im, k, n):
    k = k % n
    c, s = math.cos(2 * math.pi * k / n), math.sin(2 * math.pi * k / n)
    if k == 0:
        return re, im
    if 4 * k == n:
        return im, -re
    if im is None:
        return re * np.float32(c), re * np.float32(-s)
    if 8 * k == n:
        h = np.float32(math.sqrt(0.5))
        return (re + im) * h, (im - re) * h
    if 8 * k == 3 * n:
        h = np.float32(math.sqrt(0.5))
        return (im - re) * h, (re + im) * -h
    return re * np.float32(c) + im * np.float32(s), im * np.float32(c) - re * np.float32(s)


def plus(a, b):
    return b if a is None else a if b is None else a + b


def minus(a, b):
    return a if b is None else -b if a is None else a - b


def real_dft(x):
    n = len(x)
    if n == 1:
        return [(x[0], None)]
    if n == 2:
        return [(x[0] + x[1], None), (x[0] - x[1], None)]
    even, odd = real_dft(x[0::2]), real_dft(x[1::2])
    out = [None] * (n // 2 + 1)
    for k in range(n // 4 + 1):
        (er, ei), (orr, oi) = even[k], odd[k]
        if 4 * k == n:
            tr, ti = None, (None if orr is None else -orr)
        else:
            tr, ti = spin(orr, oi, k, n)
        out[k] = (plus(er, tr), plus(ei, ti))
        if n // 2 - k != k:
            low = minus(ei, ti)
            out[n // 2 - k] = (minus(er, tr), None if low is None else minus(None, low))
    return out


def first_table():
    half = RADIX // 2
    p, s, u0 = np.meshgrid(
        np.arange(half), np.arange(2), np.arange(GRID // 2 // RADIX), indexing="ij"
    )
    u1 = np.where(s == 0, p, np.where(p == 0, half, RADIX - p))
    u = RADIX * u0 + u1
    x0 = np.arange(LANES)
    angle = 2 * np.pi * ((u[..., None] * x0) % GRID) / GRID
    c, n = np.cos(angle) / math.sqrt(GRID), np.sin(angle) / math.sqrt(GRID)
    first = (p == 0)[..., None]
    side = (s == 0)[..., None]
    sign = np.where(side, 1.0, -1.0)
    rr = np.where(first, np.where(side, c, 0.0), c)
    ri = np.where(first, np.where(side, 0.0, c), sign * n)
    ir = np.where(first, np.where(side, -n, 0.0), -n)
    ii = np.where(first, np.where(side, 0.0, -n), sign * c)
    real = np.concatenate([rr, ri], axis=-1)
    imag = np.concatenate([ir, ii], axis=-1)
    both = np.stack([real, imag], axis=1)
    return both.reshape(half, 2 * GRID // RADIX, 2 * LANES).astype(np.float32).astype(BF16)


def turn_table():
    angle = 2 * np.pi * (np.outer(np.arange(LANES), np.arange(LANES)) % LANES) / LANES
    return np.stack([np.cos(angle), np.sin(angle)]).astype(np.float32)


def mix_table(group):
    y = np.arange(group * LANES).reshape(group, LANES, 1)
    angle = 2 * np.pi * ((y * np.arange(RADIX)) % GRID) / GRID
    c, n = np.cos(angle) / math.sqrt(GRID), np.sin(angle) / math.sqrt(GRID)
    top = np.concatenate([c, -n], axis=2)
    low = np.concatenate([n, c], axis=2)
    both = np.concatenate([top, low], axis=1)
    return np.tile(both, (1, 1, LANES // (2 * RADIX))).astype(np.float32).astype(BF16)


def dot(a, b, dims=((1,), (0,))):
    return lax.dot_general(a, b, (dims, ((), ())), preferred_element_type=F32)


def iota(shape, dim):
    return lax.broadcasted_iota(jnp.int32, shape, dim)


def ask_body(owner_ref, local_ref, sky_any, asked_ref, first_ref, last_ref, sems):
    strip, width = sky_any.shape[1], first_ref.shape[1]
    first = pltpu.make_async_copy(sky_any.at[:, pl.ds(0, width)], first_ref, sems.at[0])
    last = pltpu.make_async_copy(sky_any.at[:, pl.ds(strip - width, width)], last_ref, sems.at[1])
    first.start()
    last.start()
    number = owner_ref[...] * (8 * LANES) + local_ref[...]
    asked_ref[...] = jnp.broadcast_to(number, asked_ref.shape)
    first.wait()
    last.wait()


def plan_body(
    owner_ref, count_ref, sky_any, pattern_any, table_any,
    put_ref, live_ref, sky_ref, pattern_ref, table_ref, sems,
):
    copies = [
        pltpu.make_async_copy(source, target, sems.at[i])
        for i, (source, target) in enumerate(
            [(sky_any, sky_ref), (pattern_any, pattern_ref), (table_any, table_ref)]
        )
    ]
    for copy in copies:
        copy.start()
    n = owner_ref.shape[1]
    wide, rows = put_ref.shape
    cap = wide // (2 * GRID // LANES)
    owner_row = owner_ref[...].astype(F32)
    count_row = count_ref[...].astype(F32)
    eye = iota((n, n), 0) == iota((n, n), 1)
    owner_col = jnp.sum(jnp.where(eye, owner_row, 0.0), axis=1, keepdims=True)
    after = jnp.where((owner_col == owner_row) & (iota((n, n), 1) < iota((n, n), 0)), 1.0, 0.0)
    slot_col = jnp.sum(after, axis=1, keepdims=True)
    target_col = owner_col * float(2 * cap) + slot_col
    spread = jnp.where(iota((n, rows), 1) // 2 == iota((n, rows), 0), 1.0, 0.0)
    row = jnp.sum(spread * target_col, axis=0, keepdims=True)
    row = row + (iota((1, rows), 1) % 2 * cap).astype(F32)
    put_ref[...] = jnp.where(iota((wide, rows), 0).astype(F32) == row, 1.0, 0.0).astype(BF16)
    double = jnp.where(iota((rows, n), 0) // 2 == iota((rows, n), 1), 1.0, 0.0)
    count = jnp.sum(double * count_row, axis=1, keepdims=True)
    live_ref[...] = jnp.where(iota(live_ref.shape, 1).astype(F32) < count, 1.0, 0.0)
    for copy in copies:
        copy.wait()


def sky_body(
    me_ref, asked_ref, low_ref, sky_ref, high_ref, pattern_ref, table_ref, turn_any, mix_any,
    out_any, mid_ref, half_ref, left_ref, turn_ref, mix_ref, wide_ref, out_ref, number_ref, asked_smem, sems,
):
    asked = asked_ref[...]
    number_ref[...] = (lax.shift_right_logical(asked, 7) * (16 * LANES)) | (asked & (LANES - 1))
    ids = pltpu.make_async_copy(number_ref, asked_smem, sems.at[0])
    turn = pltpu.make_async_copy(turn_any, turn_ref, sems.at[1])
    mix = pltpu.make_async_copy(mix_any.at[me_ref[0]], mix_ref, sems.at[2])
    for copy in (ids, turn, mix):
        copy.start()
    rows = sky_ref.shape[0]
    block = 16
    for start in range(0, rows, block):
        at = slice(start, start + block)
        parts = []
        for x1 in range(RADIX):
            lo = x1 * LANES
            if lo < HALO:
                sky = low_ref[at, lo : lo + LANES]
            elif lo < GRID - HALO:
                sky = sky_ref[at, lo - HALO : lo - HALO + LANES]
            else:
                sky = high_ref[at, lo - GRID + HALO : lo - GRID + HALO + LANES]
            seen = pattern_ref[at, lo : lo + LANES].astype(F32) * sky.astype(F32)
            parts.append(seen.astype(BF16).astype(F32))
        out = real_dft(parts)
        mid_ref[0, at, :LANES] = out[0][0].astype(BF16)
        mid_ref[0, at, LANES:] = out[RADIX // 2][0].astype(BF16)
        for p in range(1, RADIX // 2):
            mid_ref[p, at, :LANES] = out[p][0].astype(BF16)
            mid_ref[p, at, LANES:] = out[p][1].astype(BF16)
    per = GRID // 2 // RADIX
    for p in range(RADIX // 2):
        half = dot(table_ref[p], mid_ref[p], ((1,), (1,))).astype(BF16).astype(F32)
        for c in range(2):
            for s in range(2):
                i = p if s == 0 else (8 - p) % 8
                first = (2 * c + s) * per
                half_ref[pl.ds(16 * s + 8 * c + i, per, stride=32), :] = half[first : first + per]
    mix.wait()
    quarter = LANES // 4
    for q in range(4):
        held = mix_ref[...].astype(F32)
        lane = iota(held.shape, 1) // quarter == q
        wide_ref[2 * LANES * q : 2 * LANES * (q + 1), :] = jnp.where(lane, held, 0.0).astype(BF16)
    ids.wait()
    turn.wait()
    group, vis = asked_ref.shape

    def step(dest, carry):
        for n in range(vis // 8):
            both = []
            for r in range(8):
                number = asked_smem[dest, 8 * n + r]
                at = pl.multiple_of(lax.shift_right_logical(number, 7), 16)
                v0 = number & (LANES - 1)
                re, im = half_ref[pl.ds(at, 8), :], half_ref[pl.ds(at + 8, 8), :]
                c, s = turn_ref[0, pl.ds(v0, 1), :], turn_ref[1, pl.ds(v0, 1), :]
                both.append((re * c + im * s, im * c - re * s))
            at = pl.ds(pl.multiple_of(dest * (2 * vis), 2 * vis) + 16 * n, 16)
            for q in range(4):
                for part in range(2):
                    lo = (2 * q + part) * LANES
                    pair = jnp.concatenate([both[q][part], both[q + 4][part]], axis=0)
                    left_ref[at, lo : lo + LANES] = pair.astype(BF16)
        return carry

    lax.fori_loop(0, group, step, 0)
    copies = []
    chunk = 256
    for i in range(group * vis * 2 // chunk):
        at = pl.ds(i * chunk, chunk)
        out_ref[at, :] = dot(left_ref[at, :], wide_ref[...]).astype(BF16)
        copies.append(pltpu.make_async_copy(out_ref.at[at], out_any.at[at], sems.at[3 + i]))
        copies[-1].start()
    for copy in copies:
        copy.wait()


def target_body(me_ref, asked_ref, kernel_any, target_ref, kernel_ref, sem):
    copy = pltpu.make_async_copy(kernel_any, kernel_ref, sem)
    copy.start()
    group, n = asked_ref.shape
    wide = target_ref.shape[1]
    cap = wide // (2 * group)
    asked = asked_ref[...]
    each = LANES * 8
    mine = asked // each == me_ref[0]
    local = (asked % each).astype(F32)
    before = jnp.where(iota((n, n), 0) < iota((n, n), 1), 1.0, 0.0).astype(BF16)
    slot = dot(jnp.where(mine, 1.0, 0.0).astype(BF16), before)
    lane = iota((group, wide), 1)
    found = jnp.zeros((group, wide), F32)
    for k in range(cap):
        hit = jnp.where(mine & (slot == float(k)), local + 1.0, 0.0)
        found = jnp.where(lane % cap == k, jnp.sum(hit, axis=1, keepdims=True), found)
    found = 2.0 * (found - 1.0) + (lane // cap % 2).astype(F32)
    own = lane // (2 * cap) == iota((group, wide), 0)
    target_ref[...] = jnp.sum(jnp.where(own, found, 0.0), axis=0, keepdims=True).astype(jnp.int32)
    copy.wait()


def swap_blocks(x):
    sub, block = iota(x.shape, 0), iota(x.shape, 1) // RADIX
    for bit in (1, 2, 4):
        up = pltpu.roll(pltpu.roll(x, 8 - bit, 0), RADIX * bit, 1)
        down = pltpu.roll(pltpu.roll(x, bit, 0), LANES - RADIX * bit, 1)
        s, b = sub & bit, block & bit
        x = jnp.where(s == b, x, jnp.where(s == 0, up, down))
    return x


def visit_body(tiles_ref, put_ref, live_ref, seen_ref, kernel_ref, res_ref, out_ref):
    cells = kernel_ref.shape[1]
    rows = seen_ref.shape[0]
    of = iota((8, cells), 0) // 2

    def left(own, h):
        return jnp.concatenate(
            [jnp.where(of == 2 * h + q, own, 0.0) for q in range(2)], axis=1
        ).astype(BF16)

    blocks = range(rows // 8)
    guesses = []
    for g in blocks:
        at = slice(8 * g, 8 * g + 8)
        total = tiles_ref[0, at].astype(F32)
        for source in range(1, tiles_ref.shape[0]):
            total = total + tiles_ref[source, at].astype(F32)
        own = swap_blocks(total.astype(BF16).astype(F32))
        guess = None
        for h in range(2):
            first = (4 * g + 2 * h) * cells
            right = jnp.concatenate(
                [kernel_ref[first : first + cells], kernel_ref[first + cells : first + 2 * cells]],
                axis=1,
            )
            guess = plus(guess, dot(left(own, h), right, ((1,), (1,))))
        guesses.append(guess)
    res = jnp.where(live_ref[...] > 0.0, seen_ref[...] - jnp.concatenate(guesses, axis=0), 0.0)
    res_ref[...] = res
    terms = []
    for g in blocks:
        own = res[8 * g : 8 * g + 8]
        term = None
        for h in range(2):
            first = (4 * g + 2 * h) * cells
            term = plus(term, dot(left(own, h), kernel_ref[first : first + 2 * cells]))
        terms.append(term)
    term = jnp.concatenate(terms, axis=0).astype(BF16)
    out_ref[...] = dot(put_ref[...], term).astype(BF16)


def dirty_body(term_ref, target_ref, out_any, out_ref, sems):
    rows = out_ref.shape[0]
    step = rows // sems.shape[0]
    target = target_ref[...]
    term = term_ref[...]
    copies = []
    for i in range(sems.shape[0]):
        at = pl.ds(i * step, step)
        hot = jnp.where(iota((step, target.shape[1]), 0) + i * step == target, 1.0, 0.0)
        out_ref[at, :] = dot(hot.astype(BF16), term)
        copies.append(pltpu.make_async_copy(out_ref.at[at], out_any.at[at], sems.at[i]))
        copies[-1].start()
    for copy in copies:
        copy.wait()


FAST = pltpu.VMEM
ANY = pl.ANY


def call(body, outs, args, scratch=()):
    shapes = [
        pltpu.VMEM(s, d) if space is FAST else jax.ShapeDtypeStruct(s, d) for s, d, space in outs
    ]
    spec = lambda space: pl.BlockSpec(memory_space=pltpu.VMEM if space is None else space)
    return pl.pallas_call(
        body,
        out_shape=shapes,
        in_specs=[spec(space) for _, space in args],
        out_specs=[spec(space) for _, _, space in outs],
        scratch_shapes=list(scratch),
    )(*[pltpu.with_memory_space_constraint(a, FAST) if space is FAST else a for a, space in args])


def exchange(block):
    return lax.all_to_all(block, GROUP_AXES, split_axis=0, concat_axis=0, tiled=True)


def on_device(sky_model, beam_pattern, kernels, observed, tile_owner, tile_local, vis_count):
    group = lax.axis_size(GROUP_AXES)
    rows, strip = sky_model.shape
    vis, cells = kernels.shape[1], kernels.shape[3]
    cap = max(2, 2 * vis // group)
    u_rows = GRID // 2 // group
    tiles_dev = u_rows // 8 * (GRID // 16)
    sem = pltpu.SemaphoreType.DMA
    me = lax.axis_index(GROUP_AXES).astype(jnp.int32).reshape(1)

    owners = tile_owner[:, :, 0]
    asking, first, last = call(
        ask_body,
        [
            ((group, vis), jnp.int32, None),
            ((rows, HALO), BF16, FAST),
            ((rows, HALO), BF16, FAST),
        ],
        [(owners, None), (tile_local, None), (sky_model, ANY)],
        [sem((2,))],
    )
    asked = exchange(asking)
    count = lax.axis_size("beam")
    forward = [(i, i + 1) for i in range(count - 1)]
    backward = [(target, source) for source, target in forward]
    low = lax.ppermute(last, "beam", forward)
    high = lax.ppermute(first, "beam", backward)

    table = first_table()
    put, live, sky_fast, pattern_fast, table_fast = call(
        plan_body,
        [
            ((2 * group * cap, 2 * vis), BF16, FAST),
            ((2 * vis, cells), F32, FAST),
            ((rows, strip), BF16, FAST),
            ((rows, GRID), BF16, FAST),
            (table.shape, BF16, FAST),
        ],
        [
            (owners, None),
            (vis_count, None),
            (sky_model, ANY),
            (beam_pattern[0], ANY),
            (table, ANY),
        ],
        [sem((3,))],
    )
    turn, mix = turn_table(), mix_table(group)
    (partial,) = call(
        sky_body,
        [((group * 2 * vis, cells), BF16, ANY)],
        [
            (me, pltpu.SMEM),
            (asked, FAST),
            (low, FAST),
            (sky_fast, FAST),
            (high, FAST),
            (pattern_fast, FAST),
            (table_fast, FAST),
            (turn, ANY),
            (mix, ANY),
        ],
        [
            pltpu.VMEM((RADIX // 2, rows, 2 * LANES), BF16),
            pltpu.VMEM((GRID, LANES), F32),
            pltpu.VMEM((group * 2 * vis, 8 * LANES), BF16),
            pltpu.VMEM(turn.shape, F32),
            pltpu.VMEM(mix.shape[1:], BF16),
            pltpu.VMEM((8 * LANES, LANES), BF16),
            pltpu.VMEM((group * 2 * vis, cells), BF16),
            pltpu.VMEM((group, vis), jnp.int32),
            pltpu.SMEM((group, vis), jnp.int32),
            sem((3 + group * 2 * vis // 256,)),
        ],
    )
    tiles = exchange(partial.reshape(group, 2 * vis, cells))
    target, kernels_fast = call(
        target_body,
        [((1, 2 * group * cap), jnp.int32, FAST), ((vis * cells, cells), BF16, FAST)],
        [(me, pltpu.SMEM), (asked, FAST), (kernels.reshape(vis * cells, cells), ANY)],
        [sem],
    )
    residual, terms = call(
        visit_body,
        [((2 * vis, cells), F32, None), ((2 * group * cap, cells), BF16, None)],
        [
            (tiles, FAST),
            (put, FAST),
            (live, FAST),
            (observed.reshape(2 * vis, cells), FAST),
            (kernels_fast, FAST),
        ],
    )
    arrived = exchange(terms.reshape(group, 2 * cap, cells))
    (dirty,) = call(
        dirty_body,
        [((2 * tiles_dev, cells), F32, ANY)],
        [(arrived.reshape(2 * group * cap, cells), FAST), (target, FAST)],
        [pltpu.VMEM((2 * tiles_dev, cells), F32), sem((8,))],
    )
    return residual.reshape(1, vis, 2, cells), dirty.reshape(1, tiles_dev, 2, cells)


def solution(mesh):
    placed = (
        P(("tile", "bl", "pol"), "beam"),
        P(("tile", "beam"), ("bl", "pol"), None),
        P(("tile", "beam"), ("bl", "pol"), None, None),
        P(("tile", "beam"), ("bl", "pol"), None, None),
        P(("tile", "beam"), ("bl", "pol"), None),
        P(("tile", "beam"), ("bl", "pol")),
        P(("tile", "beam"), ("bl", "pol")),
    )
    return jax.shard_map(
        on_device,
        mesh=mesh,
        in_specs=placed,
        out_specs=(
            P(("tile", "beam"), ("bl", "pol"), None, None),
            P(("tile", "beam"), ("bl", "pol"), None, None),
        ),
        check_vma=False,
    )
```

```python
import functools
import math

import jax
import jax.numpy as jnp
import numpy as np
from jax import lax
from jax.experimental import pallas as pl
from jax.experimental.pallas import tpu as pltpu
from jax.sharding import PartitionSpec as P

GRID = 2048
HALO = 512
RADIX = 16
LANES = GRID // RADIX
GROUP_AXES = ("bl", "pol")
F32 = jnp.float32
BF16 = jnp.bfloat16


def spin(re, im, k, n):
    k = k % n
    c, s = math.cos(2 * math.pi * k / n), math.sin(2 * math.pi * k / n)
    if k == 0:
        return re, im
    if 4 * k == n:
        return im, -re
    if im is None:
        return re * np.float32(c), re * np.float32(-s)
    if 8 * k == n:
        h = np.float32(math.sqrt(0.5))
        return (re + im) * h, (im - re) * h
    if 8 * k == 3 * n:
        h = np.float32(math.sqrt(0.5))
        return (im - re) * h, (re + im) * -h
    return re * np.float32(c) + im * np.float32(s), im * np.float32(c) - re * np.float32(s)


def plus(a, b):
    return b if a is None else a if b is None else a + b


def minus(a, b):
    return a if b is None else -b if a is None else a - b


def real_dft(x):
    n = len(x)
    if n == 1:
        return [(x[0], None)]
    if n == 2:
        return [(x[0] + x[1], None), (x[0] - x[1], None)]
    even, odd = real_dft(x[0::2]), real_dft(x[1::2])
    out = [None] * (n // 2 + 1)
    for k in range(n // 4 + 1):
        (er, ei), (orr, oi) = even[k], odd[k]
        if 4 * k == n:
            tr, ti = None, (None if orr is None else -orr)
        else:
            tr, ti = spin(orr, oi, k, n)
        out[k] = (plus(er, tr), plus(ei, ti))
        if n // 2 - k != k:
            low = minus(ei, ti)
            out[n // 2 - k] = (minus(er, tr), None if low is None else minus(None, low))
    return out


def first_table():
    half = RADIX // 2
    p, s, u0 = np.meshgrid(
        np.arange(half), np.arange(2), np.arange(GRID // 2 // RADIX), indexing="ij"
    )
    u1 = np.where(s == 0, p, np.where(p == 0, half, RADIX - p))
    u = RADIX * u0 + u1
    x0 = np.arange(LANES)
    angle = 2 * np.pi * ((u[..., None] * x0) % GRID) / GRID
    c, n = np.cos(angle) / math.sqrt(GRID), np.sin(angle) / math.sqrt(GRID)
    first = (p == 0)[..., None]
    side = (s == 0)[..., None]
    sign = np.where(side, 1.0, -1.0)
    rr = np.where(first, np.where(side, c, 0.0), c)
    ri = np.where(first, np.where(side, 0.0, c), sign * n)
    ir = np.where(first, np.where(side, -n, 0.0), -n)
    ii = np.where(first, np.where(side, 0.0, -n), sign * c)
    real = np.concatenate([rr, ri], axis=-1)
    imag = np.concatenate([ir, ii], axis=-1)
    both = np.stack([real, imag], axis=1)
    return both.reshape(half, 2 * GRID // RADIX, 2 * LANES).astype(np.float32).astype(BF16)


def turn_table():
    angle = 2 * np.pi * (np.outer(np.arange(LANES), np.arange(LANES)) % LANES) / LANES
    return np.stack([np.cos(angle), np.sin(angle)]).astype(np.float32)


def mix_table(group):
    y = np.arange(group * LANES).reshape(group, LANES, 1)
    angle = 2 * np.pi * ((y * np.arange(RADIX)) % GRID) / GRID
    c, n = np.cos(angle) / math.sqrt(GRID), np.sin(angle) / math.sqrt(GRID)
    top = np.concatenate([c, -n], axis=2)
    low = np.concatenate([n, c], axis=2)
    both = np.concatenate([top, low], axis=1)
    return np.tile(both, (1, 1, LANES // (2 * RADIX))).astype(np.float32).astype(BF16)


def dot(a, b, dims=((1,), (0,))):
    return lax.dot_general(a, b, (dims, ((), ())), preferred_element_type=F32)


def iota(shape, dim):
    return lax.broadcasted_iota(jnp.int32, shape, dim)


def ask_body(owner_ref, local_ref, asked_ref):
    number = owner_ref[...] * (8 * LANES) + local_ref[...]
    asked_ref[...] = jnp.broadcast_to(number, asked_ref.shape)


def plan_body(
    owner_ref, count_ref, sky_any, pattern_any, put_ref, live_ref, sky_ref, pattern_ref, sems
):
    copies = [
        pltpu.make_async_copy(source, target, sems.at[i])
        for i, (source, target) in enumerate(
            [(sky_any, sky_ref), (pattern_any, pattern_ref)]
        )
    ]
    for copy in copies:
        copy.start()
    n = owner_ref.shape[1]
    wide, rows = put_ref.shape
    cap = wide // (2 * GRID // LANES)
    owner_row = owner_ref[...].astype(F32)
    count_row = count_ref[...].astype(F32)
    eye = iota((n, n), 0) == iota((n, n), 1)
    owner_col = jnp.sum(jnp.where(eye, owner_row, 0.0), axis=1, keepdims=True)
    after = jnp.where((owner_col == owner_row) & (iota((n, n), 1) < iota((n, n), 0)), 1.0, 0.0)
    slot_col = jnp.sum(after, axis=1, keepdims=True)
    target_col = owner_col * float(2 * cap) + slot_col
    spread = jnp.where(iota((n, rows), 1) // 2 == iota((n, rows), 0), 1.0, 0.0)
    row = jnp.sum(spread * target_col, axis=0, keepdims=True)
    row = row + (iota((1, rows), 1) % 2 * cap).astype(F32)
    put_ref[...] = jnp.where(iota((wide, rows), 0).astype(F32) == row, 1.0, 0.0).astype(BF16)
    double = jnp.where(iota((rows, n), 0) // 2 == iota((rows, n), 1), 1.0, 0.0)
    count = jnp.sum(double * count_row, axis=1, keepdims=True)
    live_ref[...] = jnp.where(iota(live_ref.shape, 1).astype(F32) < count, 1.0, 0.0)
    for copy in copies:
        copy.wait()


def sky_body(
    low_ref, sky_ref, high_ref, pattern_ref, table_any, out_ref, mid_ref, half_ref, table_ref, sem
):
    copy = pltpu.make_async_copy(table_any, table_ref, sem)
    copy.start()
    rows = sky_ref.shape[0]
    block = 16
    for start in range(0, rows, block):
        at = slice(start, start + block)
        parts = []
        for x1 in range(RADIX):
            lo = x1 * LANES
            if lo < HALO:
                sky = low_ref[at, lo : lo + LANES]
            elif lo < GRID - HALO:
                sky = sky_ref[at, lo - HALO : lo - HALO + LANES]
            else:
                sky = high_ref[at, lo - GRID + HALO : lo - GRID + HALO + LANES]
            seen = pattern_ref[at, lo : lo + LANES].astype(F32) * sky.astype(F32)
            parts.append(seen.astype(BF16).astype(F32))
        out = real_dft(parts)
        mid_ref[0, at, :LANES] = out[0][0].astype(BF16)
        mid_ref[0, at, LANES:] = out[RADIX // 2][0].astype(BF16)
        for p in range(1, RADIX // 2):
            mid_ref[p, at, :LANES] = out[p][0].astype(BF16)
            mid_ref[p, at, LANES:] = out[p][1].astype(BF16)
    per = GRID // 2 // RADIX
    copy.wait()
    for p in range(RADIX // 2):
        half = dot(table_ref[p], mid_ref[p], ((1,), (1,)))
        for c in range(2):
            for s in range(2):
                i = p if s == 0 else (8 - p) % 8
                first = (2 * c + s) * per
                half_ref[pl.ds(16 * s + 8 * c + i, per, stride=32), :] = half[first : first + per]
    out_ref[...] = half_ref[...].astype(BF16)


def share_body(
    me_ref, asked_ref, half_ref, turn_any, mix_any, *rest, partner
):
    if partner:
        sum_ref, out_any = rest[:2]
        rest = rest[2:]
    else:
        out_any = rest[0]
        rest = rest[1:]
    left_ref, turn_ref, mix_ref, wide_ref, out_ref, number_ref, asked_smem, sems = rest
    me = me_ref[0]
    asked = asked_ref[...]
    number_ref[...] = (lax.shift_right_logical(asked, 7) * (16 * LANES)) | (asked & (LANES - 1))
    ids = pltpu.make_async_copy(number_ref, asked_smem, sems.at[0])
    turn = pltpu.make_async_copy(turn_any, turn_ref, sems.at[1])
    source = me ^ 1 if partner else me
    mix = pltpu.make_async_copy(mix_any.at[source], mix_ref, sems.at[2])
    for copy in (ids, turn, mix):
        copy.start()
    for copy in (ids, turn, mix):
        copy.wait()
    quarter = LANES // 4
    for q in range(4):
        held = mix_ref[...].astype(F32)
        lane = iota(held.shape, 1) // quarter == q
        wide_ref[2 * LANES * q : 2 * LANES * (q + 1), :] = jnp.where(lane, held, 0.0).astype(BF16)
    group, vis = asked_ref.shape
    parity = me & 1

    def step(pair, carry):
        dest = 2 * pair + parity
        for n in range(vis // 8):
            both = []
            for r in range(8):
                number = asked_smem[dest, 8 * n + r]
                at = pl.multiple_of(lax.shift_right_logical(number, 7), 16)
                v0 = number & (LANES - 1)
                cells = half_ref[pl.ds(at, 16), :].astype(F32)
                re, im = cells[:8], cells[8:]
                c, s = turn_ref[0, pl.ds(v0, 1), :], turn_ref[1, pl.ds(v0, 1), :]
                both.append((re * c + im * s, im * c - re * s))
            at = pl.ds(pl.multiple_of(pair * (2 * vis), 2 * vis) + 16 * n, 16)
            for q in range(4):
                for part in range(2):
                    lo = (2 * q + part) * LANES
                    two = jnp.concatenate([both[q][part], both[q + 4][part]], axis=0)
                    left_ref[at, lo : lo + LANES] = two.astype(BF16)
        return carry

    lax.fori_loop(0, group // 2, step, 0)
    if not partner:
        out_any[...] = dot(left_ref[...], wide_ref[...])
        return
    copies = []
    chunk = 256
    for i in range(group * vis // chunk):
        at = pl.ds(i * chunk, chunk)
        out_ref[at, :] = (sum_ref[at, :] + dot(left_ref[at, :], wide_ref[...])).astype(BF16)
        copies.append(pltpu.make_async_copy(out_ref.at[at], out_any.at[at], sems.at[3 + i]))
        copies[-1].start()
    for copy in copies:
        copy.wait()


def target_body(me_ref, asked_ref, kernel_any, target_ref, kernel_ref, sem):
    copy = pltpu.make_async_copy(kernel_any, kernel_ref, sem)
    copy.start()
    group, n = asked_ref.shape
    wide = target_ref.shape[1]
    cap = wide // (2 * group)
    asked = asked_ref[...]
    each = LANES * 8
    mine = asked // each == me_ref[0]
    local = (asked % each).astype(F32)
    before = jnp.where(iota((n, n), 0) < iota((n, n), 1), 1.0, 0.0).astype(BF16)
    slot = dot(jnp.where(mine, 1.0, 0.0).astype(BF16), before)
    lane = iota((group, wide), 1)
    found = jnp.zeros((group, wide), F32)
    for k in range(cap):
        hit = jnp.where(mine & (slot == float(k)), local + 1.0, 0.0)
        found = jnp.where(lane % cap == k, jnp.sum(hit, axis=1, keepdims=True), found)
    found = 2.0 * (found - 1.0) + (lane // cap % 2).astype(F32)
    own = lane // (2 * cap) == iota((group, wide), 0)
    target_ref[...] = jnp.sum(jnp.where(own, found, 0.0), axis=0, keepdims=True).astype(jnp.int32)
    copy.wait()


def swap_blocks(x):
    sub, block = iota(x.shape, 0), iota(x.shape, 1) // RADIX
    for bit in (1, 2, 4):
        up = pltpu.roll(pltpu.roll(x, 8 - bit, 0), RADIX * bit, 1)
        down = pltpu.roll(pltpu.roll(x, bit, 0), LANES - RADIX * bit, 1)
        s, b = sub & bit, block & bit
        x = jnp.where(s == b, x, jnp.where(s == 0, up, down))
    return x


def visit_body(tiles_ref, put_ref, live_ref, seen_ref, kernel_ref, res_ref, out_ref):
    cells = kernel_ref.shape[1]
    rows = seen_ref.shape[0]
    of = iota((8, cells), 0) // 2

    def left(own, h):
        return jnp.concatenate(
            [jnp.where(of == 2 * h + q, own, 0.0) for q in range(2)], axis=1
        ).astype(BF16)

    blocks = range(rows // 8)
    guesses = []
    for g in blocks:
        at = slice(8 * g, 8 * g + 8)
        total = tiles_ref[0, at].astype(F32)
        for source in range(1, tiles_ref.shape[0]):
            total = total + tiles_ref[source, at].astype(F32)
        own = swap_blocks(total.astype(BF16).astype(F32))
        guess = None
        for h in range(2):
            first = (4 * g + 2 * h) * cells
            right = jnp.concatenate(
                [kernel_ref[first : first + cells], kernel_ref[first + cells : first + 2 * cells]],
                axis=1,
            )
            guess = plus(guess, dot(left(own, h), right, ((1,), (1,))))
        guesses.append(guess)
    res = jnp.where(live_ref[...] > 0.0, seen_ref[...] - jnp.concatenate(guesses, axis=0), 0.0)
    res_ref[...] = res
    terms = []
    for g in blocks:
        own = res[8 * g : 8 * g + 8]
        term = None
        for h in range(2):
            first = (4 * g + 2 * h) * cells
            term = plus(term, dot(left(own, h), kernel_ref[first : first + 2 * cells]))
        terms.append(term)
    term = jnp.concatenate(terms, axis=0).astype(BF16)
    out_ref[...] = dot(put_ref[...], term).astype(BF16)


def dirty_body(term_ref, target_ref, out_any, out_ref, sems):
    rows = out_ref.shape[0]
    step = rows // sems.shape[0]
    target = target_ref[...]
    term = term_ref[...]
    copies = []
    for i in range(sems.shape[0]):
        at = pl.ds(i * step, step)
        hot = jnp.where(iota((step, target.shape[1]), 0) + i * step == target, 1.0, 0.0)
        out_ref[at, :] = dot(hot.astype(BF16), term)
        copies.append(pltpu.make_async_copy(out_ref.at[at], out_any.at[at], sems.at[i]))
        copies[-1].start()
    for copy in copies:
        copy.wait()


FAST = pltpu.VMEM
ANY = pl.ANY


def call(body, outs, args, scratch=()):
    shapes = [
        pltpu.VMEM(s, d) if space is FAST else jax.ShapeDtypeStruct(s, d) for s, d, space in outs
    ]
    spec = lambda space: pl.BlockSpec(memory_space=pltpu.VMEM if space is None else space)
    return pl.pallas_call(
        body,
        out_shape=shapes,
        in_specs=[spec(space) for _, space in args],
        out_specs=[spec(space) for _, _, space in outs],
        scratch_shapes=list(scratch),
    )(*[pltpu.with_memory_space_constraint(a, FAST) if space is FAST else a for a, space in args])


def exchange(block, axes=GROUP_AXES):
    return lax.all_to_all(block, axes, split_axis=0, concat_axis=0, tiled=True)


def on_device(sky_model, beam_pattern, kernels, observed, tile_owner, tile_local, vis_count):
    group = lax.axis_size(GROUP_AXES)
    rows, strip = sky_model.shape
    vis, cells = kernels.shape[1], kernels.shape[3]
    cap = max(2, 2 * vis // group)
    u_rows = GRID // 2 // group
    tiles_dev = u_rows // 8 * (GRID // 16)
    sem = pltpu.SemaphoreType.DMA
    me = lax.axis_index(GROUP_AXES).astype(jnp.int32).reshape(1)

    owners = tile_owner[:, :, 0]
    (asking,) = call(
        ask_body, [((group, vis), jnp.int32, None)], [(owners, None), (tile_local, None)]
    )
    count = lax.axis_size("beam")
    forward = [(i, i + 1) for i in range(count - 1)]
    backward = [(target, source) for source, target in forward]
    low = lax.ppermute(sky_model[:, strip - HALO :], "beam", forward)
    high = lax.ppermute(sky_model[:, :HALO], "beam", backward)
    asked = exchange(asking)

    table = first_table()
    put, live, sky_fast, pattern_fast = call(
        plan_body,
        [
            ((2 * group * cap, 2 * vis), BF16, FAST),
            ((2 * vis, cells), F32, FAST),
            ((rows, strip), BF16, FAST),
            ((rows, GRID), BF16, FAST),
        ],
        [
            (owners, None),
            (vis_count, None),
            (sky_model, ANY),
            (beam_pattern[0], ANY),
        ],
        [sem((2,))],
    )
    (half,) = call(
        sky_body,
        [((GRID, LANES), BF16, FAST)],
        [(low, FAST), (sky_fast, FAST), (high, FAST), (pattern_fast, FAST), (table, ANY)],
        [
            pltpu.VMEM((RADIX // 2, rows, 2 * LANES), BF16),
            pltpu.VMEM((GRID, LANES), F32),
            pltpu.VMEM(table.shape, BF16),
            sem,
        ],
    )
    other = lax.ppermute(half, "pol", [(0, 1), (1, 0)])
    turn, mix = turn_table(), mix_table(group)
    served = group * vis
    scratch = [
        pltpu.VMEM((served, 8 * LANES), BF16),
        pltpu.VMEM(turn.shape, F32),
        pltpu.VMEM(mix.shape[1:], BF16),
        pltpu.VMEM((8 * LANES, LANES), BF16),
        pltpu.VMEM((served, cells), BF16),
        pltpu.VMEM((group, vis), jnp.int32),
        pltpu.SMEM((group, vis), jnp.int32),
        sem((3 + served // 256,)),
    ]
    (own_sum,) = call(
        functools.partial(share_body, partner=False),
        [((served, cells), F32, FAST)],
        [(me, pltpu.SMEM), (asked, FAST), (half, FAST), (turn, ANY), (mix, ANY)],
        scratch,
    )
    (partial,) = call(
        functools.partial(share_body, partner=True),
        [((served, cells), BF16, ANY)],
        [(me, pltpu.SMEM), (asked, FAST), (other, FAST), (turn, ANY), (mix, ANY), (own_sum, FAST)],
        scratch,
    )
    tiles = exchange(partial.reshape(group // 2, 2 * vis, cells), "bl")
    target, kernels_fast = call(
        target_body,
        [((1, 2 * group * cap), jnp.int32, FAST), ((vis * cells, cells), BF16, FAST)],
        [(me, pltpu.SMEM), (asked, FAST), (kernels.reshape(vis * cells, cells), ANY)],
        [sem],
    )
    residual, terms = call(
        visit_body,
        [((2 * vis, cells), F32, None), ((2 * group * cap, cells), BF16, None)],
        [
            (tiles, FAST),
            (put, FAST),
            (live, FAST),
            (observed.reshape(2 * vis, cells), FAST),
            (kernels_fast, FAST),
        ],
    )
    arrived = exchange(terms.reshape(group, 2 * cap, cells))
    (dirty,) = call(
        dirty_body,
        [((2 * tiles_dev, cells), F32, ANY)],
        [(arrived.reshape(2 * group * cap, cells), FAST), (target, FAST)],
        [pltpu.VMEM((2 * tiles_dev, cells), F32), sem((8,))],
    )
    return residual.reshape(1, vis, 2, cells), dirty.reshape(1, tiles_dev, 2, cells)


def solution(mesh):
    placed = (
        P(("tile", "bl", "pol"), "beam"),
        P(("tile", "beam"), ("bl", "pol"), None),
        P(("tile", "beam"), ("bl", "pol"), None, None),
        P(("tile", "beam"), ("bl", "pol"), None, None),
        P(("tile", "beam"), ("bl", "pol"), None),
        P(("tile", "beam"), ("bl", "pol")),
        P(("tile", "beam"), ("bl", "pol")),
    )
    return jax.shard_map(
        on_device,
        mesh=mesh,
        in_specs=placed,
        out_specs=(
            P(("tile", "beam"), ("bl", "pol"), None, None),
            P(("tile", "beam"), ("bl", "pol"), None, None),
        ),
        check_vma=False,
    )
```

```python
import math

import jax
import jax.numpy as jnp
import numpy as np
from jax import lax
from jax.experimental import pallas as pl
from jax.experimental.pallas import tpu as pltpu
from jax.sharding import PartitionSpec as P

GRID = 2048
HALO = 512
RADIX = 16
LANES = GRID // RADIX
GROUP_AXES = ("bl", "pol")
F32 = jnp.float32
BF16 = jnp.bfloat16


def spin(re, im, k, n):
    k = k % n
    c, s = math.cos(2 * math.pi * k / n), math.sin(2 * math.pi * k / n)
    if k == 0:
        return re, im
    if 4 * k == n:
        return im, -re
    if im is None:
        return re * np.float32(c), re * np.float32(-s)
    if 8 * k == n:
        h = np.float32(math.sqrt(0.5))
        return (re + im) * h, (im - re) * h
    if 8 * k == 3 * n:
        h = np.float32(math.sqrt(0.5))
        return (im - re) * h, (re + im) * -h
    return re * np.float32(c) + im * np.float32(s), im * np.float32(c) - re * np.float32(s)


def plus(a, b):
    return b if a is None else a if b is None else a + b


def minus(a, b):
    return a if b is None else -b if a is None else a - b


def real_dft(x):
    n = len(x)
    if n == 1:
        return [(x[0], None)]
    if n == 2:
        return [(x[0] + x[1], None), (x[0] - x[1], None)]
    even, odd = real_dft(x[0::2]), real_dft(x[1::2])
    out = [None] * (n // 2 + 1)
    for k in range(n // 4 + 1):
        (er, ei), (orr, oi) = even[k], odd[k]
        if 4 * k == n:
            tr, ti = None, (None if orr is None else -orr)
        else:
            tr, ti = spin(orr, oi, k, n)
        out[k] = (plus(er, tr), plus(ei, ti))
        if n // 2 - k != k:
            low = minus(ei, ti)
            out[n // 2 - k] = (minus(er, tr), None if low is None else minus(None, low))
    return out


def first_table():
    half = RADIX // 2
    p, s, u0 = np.meshgrid(
        np.arange(half), np.arange(2), np.arange(GRID // 2 // RADIX), indexing="ij"
    )
    u1 = np.where(s == 0, p, np.where(p == 0, half, RADIX - p))
    u = RADIX * u0 + u1
    x0 = np.arange(LANES)
    angle = 2 * np.pi * ((u[..., None] * x0) % GRID) / GRID
    c, n = np.cos(angle) / math.sqrt(GRID), np.sin(angle) / math.sqrt(GRID)
    first = (p == 0)[..., None]
    side = (s == 0)[..., None]
    sign = np.where(side, 1.0, -1.0)
    rr = np.where(first, np.where(side, c, 0.0), c)
    ri = np.where(first, np.where(side, 0.0, c), sign * n)
    ir = np.where(first, np.where(side, -n, 0.0), -n)
    ii = np.where(first, np.where(side, 0.0, -n), sign * c)
    real = np.concatenate([rr, ri], axis=-1)
    imag = np.concatenate([ir, ii], axis=-1)
    both = np.stack([real, imag], axis=1)
    return both.reshape(half, 2 * GRID // RADIX, 2 * LANES).astype(np.float32).astype(BF16)


def turn_table():
    angle = 2 * np.pi * (np.outer(np.arange(LANES), np.arange(LANES)) % LANES) / LANES
    return np.stack([np.cos(angle), np.sin(angle)]).astype(np.float32)


def mix_table(group):
    y = np.arange(group * LANES).reshape(group, LANES, 1)
    angle = 2 * np.pi * ((y * np.arange(RADIX)) % GRID) / GRID
    c, n = np.cos(angle) / math.sqrt(GRID), np.sin(angle) / math.sqrt(GRID)
    top = np.concatenate([c, -n], axis=2)
    low = np.concatenate([n, c], axis=2)
    both = np.concatenate([top, low], axis=1)
    return np.tile(both, (1, 1, LANES // (2 * RADIX))).astype(np.float32).astype(BF16)


def dot(a, b, dims=((1,), (0,))):
    return lax.dot_general(a, b, (dims, ((), ())), preferred_element_type=F32)


def iota(shape, dim):
    return lax.broadcasted_iota(jnp.int32, shape, dim)


def front_body(
    me_ref, owner_ref, local_ref, count_ref, sky_any, pattern_any, turn_any, mix_any,
    asked_ref, first_ref, last_ref, put_ref, live_ref, sky_ref, pattern_ref, turn_ref, mix_ref, sems,
):
    me = me_ref[0]
    strip, width = sky_any.shape[1], first_ref.shape[1]
    pairs = [
        (sky_any.at[:, pl.ds(0, width)], first_ref),
        (sky_any.at[:, pl.ds(strip - width, width)], last_ref),
        (sky_any, sky_ref),
        (pattern_any, pattern_ref),
        (turn_any, turn_ref),
        (mix_any.at[me], mix_ref.at[0]),
        (mix_any.at[me ^ 1], mix_ref.at[1]),
    ]
    copies = [pltpu.make_async_copy(a, b, sems.at[i]) for i, (a, b) in enumerate(pairs)]
    for copy in copies:
        copy.start()
    number = owner_ref[...] * (8 * LANES) + local_ref[...]
    asked_ref[...] = jnp.broadcast_to(number, asked_ref.shape)
    n = owner_ref.shape[1]
    wide, rows = put_ref.shape
    cap = wide // (2 * GRID // LANES)
    owner_row = owner_ref[...].astype(F32)
    count_row = count_ref[...].astype(F32)
    eye = iota((n, n), 0) == iota((n, n), 1)
    owner_col = jnp.sum(jnp.where(eye, owner_row, 0.0), axis=1, keepdims=True)
    after = jnp.where((owner_col == owner_row) & (iota((n, n), 1) < iota((n, n), 0)), 1.0, 0.0)
    slot_col = jnp.sum(after, axis=1, keepdims=True)
    target_col = owner_col * float(2 * cap) + slot_col
    spread = jnp.where(iota((n, rows), 1) // 2 == iota((n, rows), 0), 1.0, 0.0)
    row = jnp.sum(spread * target_col, axis=0, keepdims=True)
    row = row + (iota((1, rows), 1) % 2 * cap).astype(F32)
    put_ref[...] = jnp.where(iota((wide, rows), 0).astype(F32) == row, 1.0, 0.0).astype(BF16)
    double = jnp.where(iota((rows, n), 0) // 2 == iota((rows, n), 1), 1.0, 0.0)
    count = jnp.sum(double * count_row, axis=1, keepdims=True)
    live_ref[...] = jnp.where(iota(live_ref.shape, 1).astype(F32) < count, 1.0, 0.0)
    for copy in copies:
        copy.wait()


def sky_body(
    low_ref, sky_ref, high_ref, pattern_ref, table_any, out_ref, mid_ref, half_ref, table_ref, sem
):
    copy = pltpu.make_async_copy(table_any, table_ref, sem)
    copy.start()
    rows = sky_ref.shape[0]
    block = 16
    for start in range(0, rows, block):
        at = slice(start, start + block)
        parts = []
        for x1 in range(RADIX):
            lo = x1 * LANES
            if lo < HALO:
                sky = low_ref[at, lo : lo + LANES]
            elif lo < GRID - HALO:
                sky = sky_ref[at, lo - HALO : lo - HALO + LANES]
            else:
                sky = high_ref[at, lo - GRID + HALO : lo - GRID + HALO + LANES]
            seen = pattern_ref[at, lo : lo + LANES].astype(F32) * sky.astype(F32)
            parts.append(seen.astype(BF16).astype(F32))
        out = real_dft(parts)
        mid_ref[0, at, :LANES] = out[0][0].astype(BF16)
        mid_ref[0, at, LANES:] = out[RADIX // 2][0].astype(BF16)
        for p in range(1, RADIX // 2):
            mid_ref[p, at, :LANES] = out[p][0].astype(BF16)
            mid_ref[p, at, LANES:] = out[p][1].astype(BF16)
    per = GRID // 2 // RADIX
    copy.wait()
    for p in range(RADIX // 2):
        half = dot(table_ref[p], mid_ref[p], ((1,), (1,)))
        for c in range(2):
            for s in range(2):
                i = p if s == 0 else (8 - p) % 8
                first = (2 * c + s) * per
                half_ref[pl.ds(16 * s + 8 * c + i, per, stride=32), :] = half[first : first + per]
    out_ref[...] = half_ref[...].astype(BF16)


def share_body(
    me_ref, asked_ref, own_ref, other_ref, turn_ref, mix_ref, out_any,
    left_ref, wide_ref, out_ref, number_ref, asked_smem, sems,
):
    asked = asked_ref[...]
    number_ref[...] = (lax.shift_right_logical(asked, 7) * (16 * LANES)) | (asked & (LANES - 1))
    ids = pltpu.make_async_copy(number_ref, asked_smem, sems.at[0])
    ids.start()
    halves = (own_ref, other_ref)
    quarter = LANES // 4
    for core in range(2):
        held = mix_ref[core].astype(F32)
        for q in range(4):
            lane = iota(held.shape, 1) // quarter == q
            at = pl.ds(2 * LANES * (4 * core + q), 2 * LANES)
            wide_ref[at, :] = jnp.where(lane, held, 0.0).astype(BF16)
    ids.wait()
    group, vis = asked_ref.shape
    parity = me_ref[0] & 1

    def step(pair, carry):
        dest = 2 * pair + parity
        for n in range(vis // 8):
            both = []
            for r in range(8):
                number = asked_smem[dest, 8 * n + r]
                at = pl.multiple_of(lax.shift_right_logical(number, 7), 16)
                v0 = number & (LANES - 1)
                c, s = turn_ref[0, pl.ds(v0, 1), :], turn_ref[1, pl.ds(v0, 1), :]
                turned = []
                for half_ref in halves:
                    cells = half_ref[pl.ds(at, 16), :].astype(F32)
                    re, im = cells[:8], cells[8:]
                    turned += [re * c + im * s, im * c - re * s]
                both.append(turned)
            at = pl.ds(pl.multiple_of(pair * (2 * vis), 2 * vis) + 16 * n, 16)
            for core in range(2):
                for q in range(4):
                    for part in range(2):
                        lo = (8 * core + 2 * q + part) * LANES
                        two = [both[q][2 * core + part], both[q + 4][2 * core + part]]
                        left_ref[at, lo : lo + LANES] = jnp.concatenate(two, axis=0).astype(BF16)
        return carry

    lax.fori_loop(0, group // 2, step, 0)
    copies = []
    chunk = 256
    for i in range(group * vis // chunk):
        at = pl.ds(i * chunk, chunk)
        out_ref[at, :] = dot(left_ref[at, :], wide_ref[...]).astype(BF16)
        copies.append(pltpu.make_async_copy(out_ref.at[at], out_any.at[at], sems.at[1 + i]))
        copies[-1].start()
    for copy in copies:
        copy.wait()


def target_body(me_ref, asked_ref, kernel_any, target_ref, kernel_ref, sem):
    copy = pltpu.make_async_copy(kernel_any, kernel_ref, sem)
    copy.start()
    group, n = asked_ref.shape
    wide = target_ref.shape[1]
    cap = wide // (2 * group)
    asked = asked_ref[...]
    each = LANES * 8
    mine = asked // each == me_ref[0]
    local = (asked % each).astype(F32)
    before = jnp.where(iota((n, n), 0) < iota((n, n), 1), 1.0, 0.0).astype(BF16)
    slot = dot(jnp.where(mine, 1.0, 0.0).astype(BF16), before)
    lane = iota((group, wide), 1)
    found = jnp.zeros((group, wide), F32)
    for k in range(cap):
        hit = jnp.where(mine & (slot == float(k)), local + 1.0, 0.0)
        found = jnp.where(lane % cap == k, jnp.sum(hit, axis=1, keepdims=True), found)
    found = 2.0 * (found - 1.0) + (lane // cap % 2).astype(F32)
    own = lane // (2 * cap) == iota((group, wide), 0)
    target_ref[...] = jnp.sum(jnp.where(own, found, 0.0), axis=0, keepdims=True).astype(jnp.int32)
    copy.wait()


def swap_blocks(x):
    sub, block = iota(x.shape, 0), iota(x.shape, 1) // RADIX
    for bit in (1, 2, 4):
        up = pltpu.roll(pltpu.roll(x, 8 - bit, 0), RADIX * bit, 1)
        down = pltpu.roll(pltpu.roll(x, bit, 0), LANES - RADIX * bit, 1)
        s, b = sub & bit, block & bit
        x = jnp.where(s == b, x, jnp.where(s == 0, up, down))
    return x


def visit_body(tiles_ref, put_ref, live_ref, seen_ref, kernel_ref, res_ref, out_ref):
    cells = kernel_ref.shape[1]
    rows = seen_ref.shape[0]
    of = iota((8, cells), 0) // 2

    def left(own, h):
        return jnp.concatenate(
            [jnp.where(of == 2 * h + q, own, 0.0) for q in range(2)], axis=1
        ).astype(BF16)

    blocks = range(rows // 8)
    guesses = []
    for g in blocks:
        at = slice(8 * g, 8 * g + 8)
        total = tiles_ref[0, at].astype(F32)
        for source in range(1, tiles_ref.shape[0]):
            total = total + tiles_ref[source, at].astype(F32)
        own = swap_blocks(total.astype(BF16).astype(F32))
        guess = None
        for h in range(2):
            first = (4 * g + 2 * h) * cells
            right = jnp.concatenate(
                [kernel_ref[first : first + cells], kernel_ref[first + cells : first + 2 * cells]],
                axis=1,
            )
            guess = plus(guess, dot(left(own, h), right, ((1,), (1,))))
        guesses.append(guess)
    res = jnp.where(live_ref[...] > 0.0, seen_ref[...] - jnp.concatenate(guesses, axis=0), 0.0)
    res_ref[...] = res
    terms = []
    for g in blocks:
        own = res[8 * g : 8 * g + 8]
        term = None
        for h in range(2):
            first = (4 * g + 2 * h) * cells
            term = plus(term, dot(left(own, h), kernel_ref[first : first + 2 * cells]))
        terms.append(term)
    term = jnp.concatenate(terms, axis=0).astype(BF16)
    out_ref[...] = dot(put_ref[...], term).astype(BF16)


def dirty_body(term_ref, target_ref, out_any, out_ref, sems):
    rows = out_ref.shape[0]
    step = rows // sems.shape[0]
    target = target_ref[...]
    term = term_ref[...]
    copies = []
    for i in range(sems.shape[0]):
        at = pl.ds(i * step, step)
        hot = jnp.where(iota((step, target.shape[1]), 0) + i * step == target, 1.0, 0.0)
        out_ref[at, :] = dot(hot.astype(BF16), term)
        copies.append(pltpu.make_async_copy(out_ref.at[at], out_any.at[at], sems.at[i]))
        copies[-1].start()
    for copy in copies:
        copy.wait()


FAST = pltpu.VMEM
ANY = pl.ANY


def call(body, outs, args, scratch=()):
    shapes = [
        pltpu.VMEM(s, d) if space is FAST else jax.ShapeDtypeStruct(s, d) for s, d, space in outs
    ]
    spec = lambda space: pl.BlockSpec(memory_space=pltpu.VMEM if space is None else space)
    return pl.pallas_call(
        body,
        out_shape=shapes,
        in_specs=[spec(space) for _, space in args],
        out_specs=[spec(space) for _, _, space in outs],
        scratch_shapes=list(scratch),
    )(*[pltpu.with_memory_space_constraint(a, FAST) if space is FAST else a for a, space in args])


def exchange(block, axes=GROUP_AXES):
    return lax.all_to_all(block, axes, split_axis=0, concat_axis=0, tiled=True)


def on_device(sky_model, beam_pattern, kernels, observed, tile_owner, tile_local, vis_count):
    group = lax.axis_size(GROUP_AXES)
    rows, strip = sky_model.shape
    vis, cells = kernels.shape[1], kernels.shape[3]
    cap = max(2, 2 * vis // group)
    u_rows = GRID // 2 // group
    tiles_dev = u_rows // 8 * (GRID // 16)
    sem = pltpu.SemaphoreType.DMA
    me = lax.axis_index(GROUP_AXES).astype(jnp.int32).reshape(1)

    turn, mix = turn_table(), mix_table(group)
    asking, first, last, put, live, sky_fast, pattern_fast, turn_fast, mix_fast = call(
        front_body,
        [
            ((group, vis), jnp.int32, None),
            ((rows, HALO), BF16, FAST),
            ((rows, HALO), BF16, FAST),
            ((2 * group * cap, 2 * vis), BF16, FAST),
            ((2 * vis, cells), F32, FAST),
            ((rows, strip), BF16, FAST),
            ((rows, GRID), BF16, FAST),
            (turn.shape, F32, FAST),
            ((2,) + mix.shape[1:], BF16, FAST),
        ],
        [
            (me, pltpu.SMEM),
            (tile_owner[:, :, 0], None),
            (tile_local, None),
            (vis_count, None),
            (sky_model, ANY),
            (beam_pattern[0], ANY),
            (turn, ANY),
            (mix, ANY),
        ],
        [sem((7,))],
    )
    count = lax.axis_size("beam")
    forward = [(i, i + 1) for i in range(count - 1)]
    backward = [(target, source) for source, target in forward]
    low = lax.ppermute(last, "beam", forward)
    high = lax.ppermute(first, "beam", backward)
    asked = exchange(asking)

    table = first_table()
    (half,) = call(
        sky_body,
        [((GRID, LANES), BF16, FAST)],
        [(low, FAST), (sky_fast, FAST), (high, FAST), (pattern_fast, FAST), (table, ANY)],
        [
            pltpu.VMEM((RADIX // 2, rows, 2 * LANES), BF16),
            pltpu.VMEM((GRID, LANES), F32),
            pltpu.VMEM(table.shape, BF16),
            sem,
        ],
    )
    other = lax.ppermute(half, "pol", [(0, 1), (1, 0)])
    served = group * vis
    (partial,) = call(
        share_body,
        [((served, cells), BF16, ANY)],
        [
            (me, pltpu.SMEM),
            (asked, FAST),
            (half, FAST),
            (other, FAST),
            (turn_fast, FAST),
            (mix_fast, FAST),
        ],
        [
            pltpu.VMEM((served, 16 * LANES), BF16),
            pltpu.VMEM((16 * LANES, LANES), BF16),
            pltpu.VMEM((served, cells), BF16),
            pltpu.VMEM((group, vis), jnp.int32),
            pltpu.SMEM((group, vis), jnp.int32),
            sem((1 + served // 256,)),
        ],
    )
    tiles = exchange(partial.reshape(group // 2, 2 * vis, cells), "bl")
    target, kernels_fast = call(
        target_body,
        [((1, 2 * group * cap), jnp.int32, FAST), ((vis * cells, cells), BF16, FAST)],
        [(me, pltpu.SMEM), (asked, FAST), (kernels.reshape(vis * cells, cells), ANY)],
        [sem],
    )
    residual, terms = call(
        visit_body,
        [((2 * vis, cells), F32, None), ((2 * group * cap, cells), BF16, None)],
        [
            (tiles, FAST),
            (put, FAST),
            (live, FAST),
            (observed.reshape(2 * vis, cells), FAST),
            (kernels_fast, FAST),
        ],
    )
    arrived = exchange(terms.reshape(group, 2 * cap, cells))
    (dirty,) = call(
        dirty_body,
        [((2 * tiles_dev, cells), F32, ANY)],
        [(arrived.reshape(2 * group * cap, cells), FAST), (target, FAST)],
        [pltpu.VMEM((2 * tiles_dev, cells), F32), sem((8,))],
    )
    return residual.reshape(1, vis, 2, cells), dirty.reshape(1, tiles_dev, 2, cells)


def solution(mesh):
    placed = (
        P(("tile", "bl", "pol"), "beam"),
        P(("tile", "beam"), ("bl", "pol"), None),
        P(("tile", "beam"), ("bl", "pol"), None, None),
        P(("tile", "beam"), ("bl", "pol"), None, None),
        P(("tile", "beam"), ("bl", "pol"), None),
        P(("tile", "beam"), ("bl", "pol")),
        P(("tile", "beam"), ("bl", "pol")),
    )
    return jax.shard_map(
        on_device,
        mesh=mesh,
        in_specs=placed,
        out_specs=(
            P(("tile", "beam"), ("bl", "pol"), None, None),
            P(("tile", "beam"), ("bl", "pol"), None, None),
        ),
        check_vma=False,
    )
```

```python
import math

import jax
import jax.numpy as jnp
import numpy as np
from jax import lax
from jax.experimental import pallas as pl
from jax.experimental.pallas import tpu as pltpu
from jax.sharding import PartitionSpec as P

GRID = 2048
HALO = 512
RADIX = 16
LANES = GRID // RADIX
GROUP_AXES = ("bl", "pol")
F32 = jnp.float32
BF16 = jnp.bfloat16


def spin(re, im, k, n):
    k = k % n
    c, s = math.cos(2 * math.pi * k / n), math.sin(2 * math.pi * k / n)
    if k == 0:
        return re, im
    if 4 * k == n:
        return im, -re
    if im is None:
        return re * np.float32(c), re * np.float32(-s)
    if 8 * k == n:
        h = np.float32(math.sqrt(0.5))
        return (re + im) * h, (im - re) * h
    if 8 * k == 3 * n:
        h = np.float32(math.sqrt(0.5))
        return (im - re) * h, (re + im) * -h
    return re * np.float32(c) + im * np.float32(s), im * np.float32(c) - re * np.float32(s)


def plus(a, b):
    return b if a is None else a if b is None else a + b


def minus(a, b):
    return a if b is None else -b if a is None else a - b


def real_dft(x):
    n = len(x)
    if n == 1:
        return [(x[0], None)]
    if n == 2:
        return [(x[0] + x[1], None), (x[0] - x[1], None)]
    even, odd = real_dft(x[0::2]), real_dft(x[1::2])
    out = [None] * (n // 2 + 1)
    for k in range(n // 4 + 1):
        (er, ei), (orr, oi) = even[k], odd[k]
        if 4 * k == n:
            tr, ti = None, (None if orr is None else -orr)
        else:
            tr, ti = spin(orr, oi, k, n)
        out[k] = (plus(er, tr), plus(ei, ti))
        if n // 2 - k != k:
            low = minus(ei, ti)
            out[n // 2 - k] = (minus(er, tr), None if low is None else minus(None, low))
    return out


def first_table():
    half = RADIX // 2
    p, s, u0 = np.meshgrid(
        np.arange(half), np.arange(2), np.arange(GRID // 2 // RADIX), indexing="ij"
    )
    u1 = np.where(s == 0, p, np.where(p == 0, half, RADIX - p))
    u = RADIX * u0 + u1
    x0 = np.arange(LANES)
    angle = 2 * np.pi * ((u[..., None] * x0) % GRID) / GRID
    c, n = np.cos(angle) / math.sqrt(GRID), np.sin(angle) / math.sqrt(GRID)
    both = np.stack([c, n], axis=1)
    return both.reshape(half, 2 * GRID // RADIX, LANES).astype(np.float32).astype(BF16)


def turn_table():
    angle = 2 * np.pi * (np.outer(np.arange(LANES), np.arange(LANES)) % LANES) / LANES
    return np.stack([np.cos(angle), np.sin(angle)]).astype(np.float32)


def mix_table(group):
    y = np.arange(group * LANES).reshape(group, LANES, 1)
    angle = 2 * np.pi * ((y * np.arange(RADIX)) % GRID) / GRID
    c, n = np.cos(angle) / math.sqrt(GRID), np.sin(angle) / math.sqrt(GRID)
    top = np.concatenate([c, -n], axis=2)
    low = np.concatenate([n, c], axis=2)
    both = np.concatenate([top, low], axis=1)
    return np.tile(both, (1, 1, LANES // (2 * RADIX))).astype(np.float32).astype(BF16)


def dot(a, b, dims=((1,), (0,))):
    return lax.dot_general(a, b, (dims, ((), ())), preferred_element_type=F32)


def iota(shape, dim):
    return lax.broadcasted_iota(jnp.int32, shape, dim)


def front_body(
    me_ref, owner_ref, local_ref, count_ref, sky_any, pattern_any, turn_any, mix_any, table_any,
    asked_any, first_ref, last_ref, put_ref, live_ref, pattern_ref, turn_ref, mix_ref, table_ref,
    asked_ref, sems,
):
    me = me_ref[0]
    width = first_ref.shape[1]
    pairs = [
        (sky_any.at[:, pl.ds(0, width)], first_ref),
        (sky_any.at[:, pl.ds(width, width)], last_ref),
        (asked_ref, asked_any),
        (pattern_any, pattern_ref),
        (turn_any, turn_ref),
        (mix_any.at[me], mix_ref.at[0]),
        (mix_any.at[me ^ 1], mix_ref.at[1]),
        (table_any, table_ref),
    ]
    copies = [pltpu.make_async_copy(a, b, sems.at[i]) for i, (a, b) in enumerate(pairs)]
    for copy in copies[:2]:
        copy.start()
    number = owner_ref[...] * (8 * LANES) + local_ref[...]
    asked_ref[...] = jnp.broadcast_to(number, asked_ref.shape)
    for copy in copies[2:]:
        copy.start()
    n = owner_ref.shape[1]
    wide, rows = put_ref.shape
    cap = wide // (2 * GRID // LANES)
    owner_row = owner_ref[...].astype(F32)
    count_row = count_ref[...].astype(F32)
    eye = iota((n, n), 0) == iota((n, n), 1)
    owner_col = jnp.sum(jnp.where(eye, owner_row, 0.0), axis=1, keepdims=True)
    after = jnp.where((owner_col == owner_row) & (iota((n, n), 1) < iota((n, n), 0)), 1.0, 0.0)
    slot_col = jnp.sum(after, axis=1, keepdims=True)
    target_col = owner_col * float(2 * cap) + slot_col
    spread = jnp.where(iota((n, rows), 1) // 2 == iota((n, rows), 0), 1.0, 0.0)
    row = jnp.sum(spread * target_col, axis=0, keepdims=True)
    row = row + (iota((1, rows), 1) % 2 * cap).astype(F32)
    put_ref[...] = jnp.where(iota((wide, rows), 0).astype(F32) == row, 1.0, 0.0).astype(BF16)
    double = jnp.where(iota((rows, n), 0) // 2 == iota((rows, n), 1), 1.0, 0.0)
    count = jnp.sum(double * count_row, axis=1, keepdims=True)
    live_ref[...] = jnp.where(iota(live_ref.shape, 1).astype(F32) < count, 1.0, 0.0)
    for copy in copies:
        copy.wait()


def sky_body(*refs):
    parts_ref = refs[:4]
    pattern_ref, table_ref, out_ref, mid_ref, half_ref = refs[4:]
    rows = pattern_ref.shape[0]
    block = 16
    for start in range(0, rows, block):
        at = slice(start, start + block)
        parts = []
        for x1 in range(RADIX):
            lo = x1 * LANES
            sky = parts_ref[lo // HALO][at, lo % HALO : lo % HALO + LANES]
            seen = pattern_ref[at, lo : lo + LANES].astype(F32) * sky.astype(F32)
            parts.append(seen.astype(BF16).astype(F32))
        out = real_dft(parts)
        mid_ref[0, at, :LANES] = out[0][0].astype(BF16)
        mid_ref[0, at, LANES:] = out[RADIX // 2][0].astype(BF16)
        for p in range(1, RADIX // 2):
            mid_ref[p, at, :LANES] = out[p][0].astype(BF16)
            mid_ref[p, at, LANES:] = out[p][1].astype(BF16)
    per = GRID // 2 // RADIX
    for p in range(RADIX // 2):
        with_re = dot(table_ref[p], mid_ref[p, :, :LANES], ((1,), (1,)))
        with_im = dot(table_ref[p], mid_ref[p, :, LANES:], ((1,), (1,)))
        for s in range(2):
            cos_re, sin_re = with_re[s * per : s * per + per], with_re[(2 + s) * per :][:per]
            cos_im, sin_im = with_im[s * per : s * per + per], with_im[(2 + s) * per :][:per]
            if p == 0:
                pair = (cos_re, -sin_re) if s == 0 else (cos_im, -sin_im)
            elif s == 0:
                pair = (cos_re + sin_im, cos_im - sin_re)
            else:
                pair = (cos_re - sin_im, -cos_im - sin_re)
            i = p if s == 0 else (8 - p) % 8
            for c in range(2):
                half_ref[pl.ds(16 * s + 8 * c + i, per, stride=32), :] = pair[c]
    out_ref[...] = half_ref[...].astype(BF16)


def share_body(
    me_ref, asked_ref, own_ref, other_ref, turn_ref, mix_ref, out_any,
    left_ref, wide_ref, out_ref, number_ref, asked_smem, sems,
):
    asked = asked_ref[...]
    number_ref[...] = (lax.shift_right_logical(asked, 7) * (16 * LANES)) | (asked & (LANES - 1))
    ids = pltpu.make_async_copy(number_ref, asked_smem, sems.at[0])
    ids.start()
    halves = (own_ref, other_ref)
    quarter = LANES // 4
    for core in range(2):
        held = mix_ref[core].astype(F32)
        for q in range(4):
            lane = iota(held.shape, 1) // quarter == q
            at = pl.ds(2 * LANES * (4 * core + q), 2 * LANES)
            wide_ref[at, :] = jnp.where(lane, held, 0.0).astype(BF16)
    ids.wait()
    group, vis = asked_ref.shape
    parity = me_ref[0] & 1

    def step(pair, carry):
        dest = 2 * pair + parity
        for n in range(vis // 8):
            both = []
            for r in range(8):
                number = asked_smem[dest, 8 * n + r]
                at = pl.multiple_of(lax.shift_right_logical(number, 7), 16)
                v0 = number & (LANES - 1)
                c, s = turn_ref[0, pl.ds(v0, 1), :], turn_ref[1, pl.ds(v0, 1), :]
                turned = []
                for half_ref in halves:
                    cells = half_ref[pl.ds(at, 16), :].astype(F32)
                    re, im = cells[:8], cells[8:]
                    turned += [re * c + im * s, im * c - re * s]
                both.append(turned)
            at = pl.ds(pl.multiple_of(pair * (2 * vis), 2 * vis) + 16 * n, 16)
            for core in range(2):
                for q in range(4):
                    for part in range(2):
                        lo = (8 * core + 2 * q + part) * LANES
                        two = [both[q][2 * core + part], both[q + 4][2 * core + part]]
                        left_ref[at, lo : lo + LANES] = jnp.concatenate(two, axis=0).astype(BF16)
        return carry

    lax.fori_loop(0, group // 2, step, 0, unroll=2)
    copies = []
    chunk = 256
    for i in range(group * vis // chunk):
        at = pl.ds(i * chunk, chunk)
        out_ref[at, :] = dot(left_ref[at, :], wide_ref[...]).astype(BF16)
        copies.append(pltpu.make_async_copy(out_ref.at[at], out_any.at[at], sems.at[1 + i]))
        copies[-1].start()
    for copy in copies:
        copy.wait()


def target_body(me_ref, asked_ref, kernel_any, target_ref, kernel_ref, sem):
    copy = pltpu.make_async_copy(kernel_any, kernel_ref, sem)
    copy.start()
    group, n = asked_ref.shape
    wide = target_ref.shape[1]
    cap = wide // (2 * group)
    asked = asked_ref[...]
    each = LANES * 8
    mine = asked // each == me_ref[0]
    local = (asked % each).astype(F32)
    before = jnp.where(iota((n, n), 0) < iota((n, n), 1), 1.0, 0.0).astype(BF16)
    slot = dot(jnp.where(mine, 1.0, 0.0).astype(BF16), before)
    lane = iota((group, wide), 1)
    found = jnp.zeros((group, wide), F32)
    for k in range(cap):
        hit = jnp.where(mine & (slot == float(k)), local + 1.0, 0.0)
        found = jnp.where(lane % cap == k, jnp.sum(hit, axis=1, keepdims=True), found)
    found = 2.0 * (found - 1.0) + (lane // cap % 2).astype(F32)
    own = lane // (2 * cap) == iota((group, wide), 0)
    target_ref[...] = jnp.sum(jnp.where(own, found, 0.0), axis=0, keepdims=True).astype(jnp.int32)
    copy.wait()


def swap_blocks(x):
    sub, block = iota(x.shape, 0), iota(x.shape, 1) // RADIX
    for bit in (1, 2, 4):
        up = pltpu.roll(pltpu.roll(x, 8 - bit, 0), RADIX * bit, 1)
        down = pltpu.roll(pltpu.roll(x, bit, 0), LANES - RADIX * bit, 1)
        s, b = sub & bit, block & bit
        x = jnp.where(s == b, x, jnp.where(s == 0, up, down))
    return x


def visit_body(tiles_ref, put_ref, live_ref, seen_ref, kernel_ref, res_ref, out_ref):
    cells = kernel_ref.shape[1]
    rows = seen_ref.shape[0]
    of = iota((8, cells), 0) // 2

    def left(own, h):
        return jnp.concatenate(
            [jnp.where(of == 2 * h + q, own, 0.0) for q in range(2)], axis=1
        ).astype(BF16)

    blocks = range(rows // 8)
    guesses = []
    for g in blocks:
        at = slice(8 * g, 8 * g + 8)
        total = tiles_ref[0, at].astype(F32)
        for source in range(1, tiles_ref.shape[0]):
            total = total + tiles_ref[source, at].astype(F32)
        own = swap_blocks(total.astype(BF16).astype(F32))
        guess = None
        for h in range(2):
            first = (4 * g + 2 * h) * cells
            right = jnp.concatenate(
                [kernel_ref[first : first + cells], kernel_ref[first + cells : first + 2 * cells]],
                axis=1,
            )
            guess = plus(guess, dot(left(own, h), right, ((1,), (1,))))
        guesses.append(guess)
    res = jnp.where(live_ref[...] > 0.0, seen_ref[...] - jnp.concatenate(guesses, axis=0), 0.0)
    res_ref[...] = res
    terms = []
    for g in blocks:
        own = res[8 * g : 8 * g + 8]
        term = None
        for h in range(2):
            first = (4 * g + 2 * h) * cells
            term = plus(term, dot(left(own, h), kernel_ref[first : first + 2 * cells]))
        terms.append(term)
    term = jnp.concatenate(terms, axis=0).astype(BF16)
    out_ref[...] = dot(put_ref[...], term).astype(BF16)


def dirty_body(term_ref, target_ref, out_any, out_ref, sems):
    rows = out_ref.shape[0]
    step = rows // sems.shape[0]
    target = target_ref[...]
    term = term_ref[...]
    copies = []
    for i in range(sems.shape[0]):
        at = pl.ds(i * step, step)
        hot = jnp.where(iota((step, target.shape[1]), 0) + i * step == target, 1.0, 0.0)
        out_ref[at, :] = dot(hot.astype(BF16), term)
        copies.append(pltpu.make_async_copy(out_ref.at[at], out_any.at[at], sems.at[i]))
        copies[-1].start()
    for copy in copies:
        copy.wait()


FAST = pltpu.VMEM
ANY = pl.ANY


def call(body, outs, args, scratch=()):
    shapes = [
        pltpu.VMEM(s, d) if space is FAST else jax.ShapeDtypeStruct(s, d) for s, d, space in outs
    ]
    spec = lambda space: pl.BlockSpec(memory_space=pltpu.VMEM if space is None else space)
    return pl.pallas_call(
        body,
        out_shape=shapes,
        in_specs=[spec(space) for _, space in args],
        out_specs=[spec(space) for _, _, space in outs],
        scratch_shapes=list(scratch),
    )(*[pltpu.with_memory_space_constraint(a, FAST) if space is FAST else a for a, space in args])


def exchange(block, axes=GROUP_AXES):
    return lax.all_to_all(block, axes, split_axis=0, concat_axis=0, tiled=True)


def on_device(sky_model, beam_pattern, kernels, observed, tile_owner, tile_local, vis_count):
    group = lax.axis_size(GROUP_AXES)
    rows, _ = sky_model.shape
    vis, cells = kernels.shape[1], kernels.shape[3]
    cap = max(2, 2 * vis // group)
    u_rows = GRID // 2 // group
    tiles_dev = u_rows // 8 * (GRID // 16)
    sem = pltpu.SemaphoreType.DMA
    me = lax.axis_index(GROUP_AXES).astype(jnp.int32).reshape(1)

    turn, mix = turn_table(), mix_table(group)
    table = first_table()
    asking, first, last, put, live, pattern_fast, turn_fast, mix_fast, table_fast = call(
        front_body,
        [
            ((group, vis), jnp.int32, ANY),
            ((rows, HALO), BF16, FAST),
            ((rows, HALO), BF16, FAST),
            ((2 * group * cap, 2 * vis), BF16, FAST),
            ((2 * vis, cells), F32, FAST),
            ((rows, GRID), BF16, FAST),
            (turn.shape, F32, FAST),
            ((2,) + mix.shape[1:], BF16, FAST),
            (table.shape, BF16, FAST),
        ],
        [
            (me, pltpu.SMEM),
            (tile_owner[:, :, 0], None),
            (tile_local, None),
            (vis_count, None),
            (sky_model, ANY),
            (beam_pattern[0], ANY),
            (turn, ANY),
            (mix, ANY),
            (table, ANY),
        ],
        [pltpu.VMEM((group, vis), jnp.int32), sem((8,))],
    )
    count = lax.axis_size("beam")
    forward = [(i, i + 1) for i in range(count - 1)]
    backward = [(target, source) for source, target in forward]
    low = lax.ppermute(last, "beam", forward)
    high = lax.ppermute(first, "beam", backward)
    asked = exchange(asking)

    (half,) = call(
        sky_body,
        [((GRID, LANES), BF16, FAST)],
        [(a, FAST) for a in (low, first, last, high, pattern_fast, table_fast)],
        [
            pltpu.VMEM((RADIX // 2, rows, 2 * LANES), BF16),
            pltpu.VMEM((GRID, LANES), F32),
        ],
    )
    other = lax.ppermute(half, "pol", [(0, 1), (1, 0)])
    served = group * vis
    (partial,) = call(
        share_body,
        [((served, cells), BF16, ANY)],
        [
            (me, pltpu.SMEM),
            (asked, FAST),
            (half, FAST),
            (other, FAST),
            (turn_fast, FAST),
            (mix_fast, FAST),
        ],
        [
            pltpu.VMEM((served, 16 * LANES), BF16),
            pltpu.VMEM((16 * LANES, LANES), BF16),
            pltpu.VMEM((served, cells), BF16),
            pltpu.VMEM((group, vis), jnp.int32),
            pltpu.SMEM((group, vis), jnp.int32),
            sem((1 + served // 256,)),
        ],
    )
    tiles = exchange(partial.reshape(group // 2, 2 * vis, cells), "bl")
    target, kernels_fast = call(
        target_body,
        [((1, 2 * group * cap), jnp.int32, FAST), ((vis * cells, cells), BF16, FAST)],
        [(me, pltpu.SMEM), (asked, FAST), (kernels.reshape(vis * cells, cells), ANY)],
        [sem],
    )
    residual, terms = call(
        visit_body,
        [((2 * vis, cells), F32, None), ((2 * group * cap, cells), BF16, None)],
        [
            (tiles, FAST),
            (put, FAST),
            (live, FAST),
            (observed.reshape(2 * vis, cells), FAST),
            (kernels_fast, FAST),
        ],
    )
    arrived = exchange(terms.reshape(group, 2 * cap, cells))
    (dirty,) = call(
        dirty_body,
        [((2 * tiles_dev, cells), F32, ANY)],
        [(arrived.reshape(2 * group * cap, cells), FAST), (target, FAST)],
        [pltpu.VMEM((2 * tiles_dev, cells), F32), sem((8,))],
    )
    return residual.reshape(1, vis, 2, cells), dirty.reshape(1, tiles_dev, 2, cells)


def solution(mesh):
    placed = (
        P(("tile", "bl", "pol"), "beam"),
        P(("tile", "beam"), ("bl", "pol"), None),
        P(("tile", "beam"), ("bl", "pol"), None, None),
        P(("tile", "beam"), ("bl", "pol"), None, None),
        P(("tile", "beam"), ("bl", "pol"), None),
        P(("tile", "beam"), ("bl", "pol")),
        P(("tile", "beam"), ("bl", "pol")),
    )
    return jax.shard_map(
        on_device,
        mesh=mesh,
        in_specs=placed,
        out_specs=(
            P(("tile", "beam"), ("bl", "pol"), None, None),
            P(("tile", "beam"), ("bl", "pol"), None, None),
        ),
        check_vma=False,
    )
```
